128 devices in a mesh: gx: 8 (over y, core), gy: 16 (over z, x).
Axes of the slice: x: 4, y: 4, z: 4, core: 2. Of those that a mesh axis runs over, the one named last changes fastest.
Arguments:
- weighted_jacobian_strips: float32 [16384, 3, 768], P(('gx', 'gy')), may hold values from -0.3125 to 0.3125
- leading_pose_index: int32 [16384, 1], P(('gx', 'gy')), may hold values from 0 to 127; in each aligned block of 128 rows (0 to 127, 128 to 255, ...) at most 2 rows name the same one
- levenberg_shift: float32 [128, 768], P(('gx', 'gy')), may hold values from 0.05 to 0.5
- removal_flags: int32 [128], replicated, may hold values from 0 to 1, as said below
Outputs:
- schur: float32 [128, 3, 768, 768], P(('gx', 'gy'))
- coupling: float32 [128, 4, 768, 768], P(('gx', 'gy'))
The draws below stay inside these ranges and needn't reach their ends.
Inputs may be any that keep to these rules, and one draw needn't show every extreme that they name: `leading_pose_index`: within the 128 columns of one device no block is the base of more than 2 columns, and some device reaches 2. `removal_flags`: eliminated blocks lie 3 or more blocks apart around the cycle of 128 blocks.
All inputs are finite; a program needn't handle non-finite values.
Results may differ from the reference program's by a relative error of at most 0.0003.
Values sent between devices are 32-bit elements; how exact they have to be, the bound alone decides.
A program may use at most 192 MiB of HBM per device.

```python
import math
import jax
import jax.numpy as jnp
import numpy as np
from jax import lax

B = 768
SURF_DEV = 128
NB = 128
SURFELS = 16384
MOST = 2
N_GX = 8
N_GY = 16


def draw_removal_flags(key, part):
    key_gaps, key_start = jax.random.split(jax.random.fold_in(key, 17))
    count_all = NB // 3
    spare_gaps = NB - 3 * count_all
    shuffled = jax.random.permutation(key_gaps, count_all)
    gap_sizes = jnp.where(shuffled < spare_gaps, 4, 3).astype(jnp.int32)
    anchor = jax.random.randint(key_start, (), 0, NB, dtype=jnp.int32)
    places = (anchor + jnp.cumsum(gap_sizes) - gap_sizes) % NB
    return jnp.zeros((NB,), jnp.int32).at[places].set(1)


def level_of(own_key, dims, pieces, low, largest):
    level = 1.0
    for axis_at, blocks in pieces:
        draws = jax.random.uniform(jax.random.fold_in(jax.random.fold_in(own_key, 6), axis_at), (blocks,), jnp.float32, low / len(pieces), largest / len(pieces))
        level = level * jnp.repeat(jnp.exp(draws), dims[axis_at] // blocks).reshape((-1,) + (1,) * (len(dims) - 1 - axis_at))
    return level


def assign_block(key, own, number, rows, amount, top, reach, lean):
    sequence = jax.random.permutation(key, amount)
    crowded, usual = shares(amount, rows * top, reach, lean, True), shares(amount, rows * top, reach, lean, False)
    places = jnp.arange(amount)

    def named(sizes, turn):
        used = int((sizes > 0).sum())
        fixed = max(1, used // 4)
        passed = fixed + (places - fixed + turn * (used - fixed)) % max(1, amount - fixed)
        return jnp.zeros((amount,), jnp.int32).at[sequence[jnp.where(places < fixed, places, passed)]].set(jnp.asarray(sizes, jnp.int32))

    sizes = jnp.where(number % 4 == 0, named(crowded, number // 4), named(usual, number - number // 4 - 1))
    mixed = jax.random.permutation(jax.random.fold_in(own, 3), amount)
    giver, sink = mixed[0:amount // 2 * 2:2], mixed[1:amount // 2 * 2:2]
    room = jnp.minimum(sizes[giver] - 1, reach - sizes[sink]) // 2
    room = jnp.where((giver == sequence[0]) | (sink == sequence[0]) | (sizes[sink] == 0), 0, jnp.maximum(room, 0))
    passed = jax.random.randint(jax.random.fold_in(own, 4), (amount // 2,), 0, 1 << 20) % (room + 1)
    sizes = sizes.at[giver].add(-passed).at[sink].add(passed)
    labels = jnp.searchsorted(jnp.cumsum(sizes), jnp.arange(rows * top), side="right").astype(jnp.int32)
    table = labels.reshape(top, rows).T
    table = table[jax.random.permutation(jax.random.fold_in(own, 1), rows)]
    turn = jax.random.randint(jax.random.fold_in(own, 2), (rows, 1), 0, top)
    return jnp.take_along_axis(table, (jnp.arange(top)[None, :] + turn) % top, axis=1)


def shares(count, total, limit, slope, full):
    portions = [(1 << 20) // math.isqrt(rank ** slope) + 1 for rank in range(1, count + 1)]
    largest = limit if full else min(limit, max(-(-total // count), total * portions[0] // sum(portions)))
    least = 1 if total - largest >= count - 1 else 0
    holding, spare = [largest] + [least] * (count - 1), total - largest - least * (count - 1)
    while spare > 0:
        free = [i for i in range(1, count) if holding[i] < largest] or [i for i in range(1, count) if holding[i] < limit]
        whole, budget = sum([portions[i] for i in free]), spare
        for i in free:
            more = min(limit - holding[i], max(1, budget * portions[i] // whole), spare)
            holding[i] = holding[i] + more
            spare = spare - more
    return np.array(holding)


def centred(key, shape, scale, reach, cuts=(), kind=jnp.bfloat16):
    result = scale * jax.random.normal(key, shape, jnp.float32)
    if cuts:
        result = result * level_of(key, shape, cuts, -0.22, 0.18)
    return jnp.clip(result, -reach, reach).astype(kind)


def setup_inputs(seed: int = 0) -> dict:
    key_of = jax.random.split(jax.random.key(seed), 5)
    weighted_jacobian_strips = centred(key_of[0], (SURFELS, 3, B), (3 * SURF_DEV) ** -0.5, 0.3125, ((0, 128),), jnp.float32)
    leading_pose_index_keys = jax.random.split(jax.random.fold_in(key_of[1], 1), SURFELS // SURF_DEV)
    leading_pose_index_turns = jax.random.permutation(jax.random.fold_in(key_of[1], 3), SURFELS // SURF_DEV)
    leading_pose_index = jax.vmap(lambda own, number: assign_block(jax.random.fold_in(key_of[1], 2), own, number, SURF_DEV, NB, 1, MOST, 2))(leading_pose_index_keys, leading_pose_index_turns).reshape((SURFELS, 1))
    levenberg_shift = jnp.clip(jnp.exp(math.log(0.5) - 2.3025851 * jax.random.uniform(key_of[2], (NB, B), jnp.float32) ** level_of(key_of[2], (NB, B), ((0, 128),), -0.2, 0.2)), 0.05, 0.5)
    removal_flags = draw_removal_flags(jax.random.fold_in(key_of[4], 71), 0)
    return dict(weighted_jacobian_strips=weighted_jacobian_strips, leading_pose_index=leading_pose_index, levenberg_shift=levenberg_shift, removal_flags=removal_flags)


def pair_gram(left_op, right_op):
    return jnp.dot(left_op.T.astype(jnp.float32), right_op.astype(jnp.float32), precision=lax.Precision.HIGHEST, preferred_element_type=jnp.float32)

def batch_gram(left_op, right_op):
    return jnp.einsum('nki,nkj->nij', left_op, right_op, precision=lax.Precision.HIGHEST)

def triangular(lower_tri, right_side):
    return jax.scipy.linalg.solve_triangular(lower_tri, right_side, lower=True)

def from_block(array, step):
    return jnp.roll(array, -step, axis=0)

def reference(weighted_jacobian_strips, leading_pose_index, levenberg_shift, removal_flags):
    count_all = weighted_jacobian_strips.shape[0]
    capacity = N_GX * N_GY * MOST
    blocks = leading_pose_index[:, 0].astype(jnp.int32)
    shuffled = jnp.argsort(blocks, stable=True).astype(jnp.int32)
    sorted_blocks = blocks[shuffled]
    first_seen = jnp.searchsorted(sorted_blocks, sorted_blocks, side='left').astype(jnp.int32)
    within = jnp.arange(count_all, dtype=jnp.int32) - first_seen
    padded = jnp.zeros((NB, capacity, 3, B), jnp.float32).at[sorted_blocks, within].set(weighted_jacobian_strips[shuffled])

    def assemble(block_id):
        own_rows = padded[block_id]
        one_back = padded[(block_id - 1) % NB]
        two_back = padded[(block_id - 2) % NB]
        diag_tile = pair_gram(own_rows[:, 0], own_rows[:, 0]) + pair_gram(one_back[:, 1], one_back[:, 1])
        diag_tile = diag_tile + pair_gram(two_back[:, 2], two_back[:, 2]) + jnp.diag(levenberg_shift[block_id])
        near_tile = pair_gram(one_back[:, 0], one_back[:, 1]) + pair_gram(two_back[:, 1], two_back[:, 2])
        far_tile = pair_gram(two_back[:, 0], two_back[:, 2])
        return jnp.stack([far_tile, near_tile, diag_tile])
    tiles = lax.map(assemble, jnp.arange(NB, dtype=jnp.int32))
    far_all = tiles[:, 0]
    near_all = tiles[:, 1]
    diagonal_blocks_full = tiles[:, 2]
    factor = jnp.linalg.cholesky(diagonal_blocks_full)
    next_all = jnp.roll(near_all, -1, axis=0)
    after_all = jnp.roll(far_all, -2, axis=0)
    right_sides = jnp.concatenate([jnp.swapaxes(far_all, 1, 2), jnp.swapaxes(near_all, 1, 2), next_all, after_all], axis=2)
    solved = jax.vmap(triangular)(factor, right_sides)
    panels = [solved[:, :, member * B:(member + 1) * B] for member in range(4)]
    coupling = jnp.stack([from_block(panels[0], 2), from_block(panels[1], 1), from_block(panels[2], -1), from_block(panels[3], -2)], axis=1)
    flag_strip = removal_flags.astype(jnp.float32)[:, None, None]
    lower_two, lower_one, upper_one, upper_two = [flag_strip * system_matrix for system_matrix in panels]
    new_diag = diagonal_blocks_full - batch_gram(from_block(lower_two, 2), from_block(lower_two, 2))
    new_diag = new_diag - batch_gram(from_block(lower_one, 1), from_block(lower_one, 1))
    new_diag = new_diag - batch_gram(from_block(upper_one, -1), from_block(upper_one, -1))
    new_diag = new_diag - batch_gram(from_block(upper_two, -2), from_block(upper_two, -2))
    new_near = near_all - batch_gram(from_block(lower_two, 1), from_block(lower_one, 1))
    new_near = new_near - batch_gram(from_block(upper_one, -2), from_block(upper_two, -2))
    new_far = far_all - batch_gram(from_block(lower_one, -1), from_block(upper_one, -1))
    prior_pose_tile_single = (jnp.roll(removal_flags, 1) > 0)[:, None, None]
    prior_pose_tile_double = (jnp.roll(removal_flags, 2) > 0)[:, None, None]
    new_near = jnp.where(prior_pose_tile_single, from_block(upper_one, -1), new_near)
    new_far = jnp.where(prior_pose_tile_double, from_block(upper_two, -2), new_far)
    current_pose_tile = (removal_flags > 0)[:, None, None]
    schur = jnp.stack([jnp.where(current_pose_tile, jnp.swapaxes(panels[0], 1, 2), new_far), jnp.where(current_pose_tile, jnp.swapaxes(panels[1], 1, 2), new_near), jnp.where(current_pose_tile, factor, new_diag)], axis=1)
    return (schur, coupling)
```

```python
import jax
import jax.numpy as jnp
from jax import lax
from jax.experimental import pallas as pl
from jax.experimental.pallas import tpu as pltpu
from jax.sharding import PartitionSpec as P

F32 = jnp.float32
BF16 = jnp.bfloat16
AXES = ("gx", "gy")


def split2(x):
    hi = x.astype(BF16)
    lo = (x - hi.astype(F32)).astype(BF16)
    return hi, lo


def dg(x, y, dims=((1,), (0,))):
    return lax.dot_general(x, y, (dims, ((), ())), preferred_element_type=F32)


def dot3(x, y, dims=((1,), (0,))):
    return dg(x[0], y[0], dims) + (dg(x[0], y[1], dims) + dg(x[1], y[0], dims))


def bucket_kernel(strips_ref, col_ref, row_ref, flag_ref, first_ref, second_ref):
    n = row_ref.shape[1]
    width = strips_ref.shape[1] // 3
    row = row_ref[...]
    col = col_ref[...]
    r_id = lax.broadcasted_iota(jnp.int32, (n, n), 0)
    c_id = lax.broadcasted_iota(jnp.int32, (n, n), 1)
    same = jnp.where((col == row) & (r_id < c_id), 1, 0)
    within = jnp.sum(same, axis=0, keepdims=True)
    t_id = lax.broadcasted_iota(jnp.int32, (2 * n, n), 0)
    lane = lax.broadcasted_iota(jnp.int32, (2 * n, n), 1)
    block = t_id >> 1
    slot_ok = within == (t_id & 1)
    hit = [slot_ok & (((row + shift) & (n - 1)) == block) for shift in range(4)]
    flags = flag_ref[...]

    def flag_before(step):
        chosen = lane == ((block + (n - step)) & (n - 1))
        return jnp.sum(jnp.where(chosen, flags, 0), axis=1, keepdims=True) > 0

    one_before = flag_before(1)
    two_before = flag_before(2)

    def mask(cond):
        return jnp.where(cond, 1.0, 0.0).astype(BF16)

    pieces = []
    for i in range(3):
        x = strips_ref[:, i * width : (i + 1) * width]
        hi = x.astype(BF16)
        rest = x - hi.astype(F32)
        mid = rest.astype(BF16)
        low = (rest - mid.astype(F32)).astype(BF16)
        pieces.append((hi, mid, low))

    def pick(select, i):
        hi, mid, low = pieces[i]
        return dg(select, hi) + (dg(select, mid) + dg(select, low))

    for i in range(3):
        first_ref[:, i * width : (i + 1) * width] = pick(mask(hit[i]), i)
    second_ref[:, 0:width] = pick(mask(hit[1] & ~one_before), 0) + pick(
        mask(hit[3] & one_before), 1
    )
    second_ref[:, width : 2 * width] = pick(mask(hit[2]), 1)
    second_ref[:, 2 * width : 3 * width] = pick(mask(hit[2] & ~two_before), 0) + pick(
        mask(hit[3] & two_before), 2
    )


def bucket(strips, index, flags):
    n = strips.shape[0]
    wide = strips.shape[1] * strips.shape[2]
    shape = jax.ShapeDtypeStruct((2 * n, wide), F32)
    return pl.pallas_call(
        bucket_kernel,
        out_shape=(shape, shape),
        name="bucket",
    )(strips.reshape(n, wide), index, index.reshape(1, n), flags.reshape(1, n))


def chol_block(a):
    n = a.shape[0]
    groups = n // 8
    sub = lax.broadcasted_iota(jnp.int32, (8, n), 0)
    lane = lax.broadcasted_iota(jnp.int32, (8, n), 1)
    left = [a[8 * v : 8 * v + 8, :] for v in range(groups)]
    right = [jnp.where(lane == sub + 8 * v, 1.0, 0.0).astype(F32) for v in range(groups)]

    def lanes_of(x, k):
        return [jnp.broadcast_to(x[:, 8 * k + i : 8 * k + i + 1], (8, n)) for i in range(8)]

    def sub_of(x, i):
        return jnp.broadcast_to(x[i : i + 1, :], (8, n))

    for k in range(groups):
        c = lanes_of(left[k], k)
        u, v_in = left[k], right[k]
        scale, row_u, row_v, row_c = [], [], [], []
        for i in range(8):
            inv = lax.rsqrt(sub_of(c[i], i))
            ru = sub_of(u, i) * inv
            rv = sub_of(v_in, i) * inv
            rc = [None] * 8
            m = jnp.where(sub > i, c[i] * inv, 0.0)
            for j in range(i + 1, 8):
                rc[j] = sub_of(c[j], i) * inv
                c[j] = c[j] - m * rc[j]
            u = jnp.where(sub == i, ru, u - m * ru)
            v_in = jnp.where(sub == i, rv, v_in - m * rv)
            scale.append(inv)
            row_u.append(ru)
            row_v.append(rv)
            row_c.append(rc)
        left[k], right[k] = u, v_in
        for g in range(k + 1, groups):
            c = lanes_of(left[g], k)
            x, y = left[g], right[g]
            for i in range(8):
                m = c[i] * scale[i]
                for j in range(i + 1, 8):
                    c[j] = c[j] - m * row_c[i][j]
                x = x - m * row_u[i]
                y = y - m * row_v[i]
            left[g], right[g] = x, y
    upper = jnp.concatenate(left, axis=0)
    r_id = lax.broadcasted_iota(jnp.int32, (n, n), 0)
    c_id = lax.broadcasted_iota(jnp.int32, (n, n), 1)
    return jnp.where(c_id >= r_id, upper, 0.0), jnp.concatenate(right, axis=0)


def chol_kernel(recv_ref, shift_ref, l_ref, w0_ref, w1_ref, w2_ref, ath_ref, atl_ref, m_ref, x_ref):
    size = shift_ref.shape[1]
    slots = recv_ref.shape[0]
    nb = 128
    count = size // nb
    w_refs = (w0_ref, w1_ref, w2_ref)
    l_ref[...] = jnp.zeros_like(l_ref)
    parts = []
    for i in range(3):
        at = recv_ref[:, i * size : (i + 1) * size].T
        m_ref[:, size + i * slots : size + (i + 1) * slots] = at
        hi, lo = split2(at)
        ath_ref[:, i * slots : (i + 1) * slots] = hi
        atl_ref[:, i * slots : (i + 1) * slots] = lo
    for blk in range(0, size, 256):
        total = None
        for i in range(3):
            a = split2(recv_ref[:, i * size + blk : i * size + blk + 256])
            t = (ath_ref[:, i * slots : (i + 1) * slots], atl_ref[:, i * slots : (i + 1) * slots])
            add = dot3(t, a)
            total = add if total is None else total + add
        r_id = lax.broadcasted_iota(jnp.int32, (size, 256), 0)
        c_id = lax.broadcasted_iota(jnp.int32, (size, 256), 1) + blk
        m_ref[:, blk : blk + 256] = total + jnp.where(
            r_id == c_id, shift_ref[:, blk : blk + 256], 0.0
        )

    def step(k, carry):
        at = pl.multiple_of(k * nb, nb)
        upper, inverse = chol_block(m_ref[pl.ds(at, nb), pl.ds(at, nb)])
        l_ref[pl.ds(at, nb), pl.ds(at, nb)] = upper.T
        inv = split2(inverse)
        for blk in range(0, 2 * size, 256):
            x_ref[:, blk : blk + 256] = dot3(inv, split2(m_ref[pl.ds(at, nb), blk : blk + 256]))
        for i in range(3):
            w_refs[i][pl.ds(at, nb), :] = x_ref[:, size + i * slots : size + (i + 1) * slots]

        def trail(r, inner):
            to = pl.multiple_of(r * nb, nb)
            low = x_ref[:, pl.ds(to, nb)].T
            l_ref[pl.ds(to, nb), pl.ds(at, nb)] = low
            low = split2(low)
            for blk in range(0, 2 * size, 256):
                m_ref[pl.ds(to, nb), blk : blk + 256] -= dot3(
                    low, split2(x_ref[:, blk : blk + 256])
                )
            return inner

        return lax.fori_loop(k + 1, count, trail, carry)

    lax.fori_loop(0, count, step, 0)


def chol(recv, shift):
    size = shift.shape[1]
    slots = recv.shape[0]
    w = jax.ShapeDtypeStruct((size, slots), F32)
    half = jax.ShapeDtypeStruct((size, 3 * slots), BF16)
    return pl.pallas_call(
        chol_kernel,
        out_shape=(jax.ShapeDtypeStruct((size, size), F32), w, w, w, half, half),
        scratch_shapes=[pltpu.VMEM((size, size + 3 * slots), F32), pltpu.VMEM((128, size + 3 * slots), F32)],
        compiler_params=pltpu.CompilerParams(vmem_limit_bytes=50 * 2**20),
        name="chol",
    )(recv, shift)


def last_kernel(
    flag_ref, recv_ref, ath_ref, atl_ref, q_ref, shift_ref, l_ref, w1_ref, w2_ref,
    m1w0_ref, m1w1_ref, m2w0_ref, p1w1_ref, p1w2_ref, p2w2_ref, e_ref,
    schur_ref, coup_ref,
    qh_ref, ql_ref, wh_ref, wl_ref, wth_ref, wtl_ref, f_ref,
):
    step = pl.program_id(0)
    size = shift_ref.shape[1]
    slots = recv_ref.shape[0]
    cols = schur_ref.shape[3]
    fm2, fm1, own, fp1, fp2 = [flag_ref[i] > 0 for i in range(5)]
    w_refs = (m1w0_ref, m1w1_ref, m2w0_ref, p1w1_ref, p1w2_ref, p2w2_ref)

    @pl.when(step == 0)
    def _():
        for i in range(3):
            hi, lo = split2(q_ref[:, i * size : (i + 1) * size].T)
            qh_ref[:, i * slots : (i + 1) * slots] = hi
            ql_ref[:, i * slots : (i + 1) * slots] = lo
        for i in range(6):
            hi, lo = split2(w_refs[i][...])
            wh_ref[i] = hi
            wl_ref[i] = lo
        for i in range(7):
            hi, lo = split2((w_refs[i] if i < 6 else e_ref)[...].T)
            wth_ref[i] = hi
            wtl_ref[i] = lo

    base = pl.multiple_of(step * cols, cols)

    def a_part(i):
        return recv_ref[:, pl.ds(pl.multiple_of(i * size + base, cols), cols)]

    def w_of(i):
        return wh_ref[i], wl_ref[i]

    def wt_of(i):
        return wth_ref[i], wtl_ref[i]

    def at_of(i):
        return ath_ref[:, i * slots : (i + 1) * slots], atl_ref[:, i * slots : (i + 1) * slots]

    def q_of(i):
        return qh_ref[:, i * slots : (i + 1) * slots], ql_ref[:, i * slots : (i + 1) * slots]

    a0, a1, a2 = [split2(a_part(i)) for i in range(3)]
    coup_ref[0, 0] = dot3(w_of(5), a0)
    coup_ref[0, 1] = dot3(w_of(3), a0) + dot3(w_of(4), a1)
    coup_ref[0, 2] = dot3(w_of(0), a1) + dot3(w_of(1), a2)
    coup_ref[0, 3] = dot3(w_of(2), a2)

    @pl.when(own)
    def _():
        w1 = split2(w1_ref[pl.ds(base, cols), :])
        w2 = split2(w2_ref[pl.ds(base, cols), :])
        over = ((1,), (1,))
        schur_ref[0, 0] = dot3(q_of(2), w2, over)
        schur_ref[0, 1] = dot3(q_of(0), w1, over) + dot3(q_of(1), w2, over)
        schur_ref[0, 2] = l_ref[:, pl.ds(base, cols)]

    @pl.when(jnp.logical_not(own))
    def _():
        f_ref[...] = jnp.zeros_like(f_ref)

        @pl.when(fp2)
        def _():
            f_ref[0] = dot3(wt_of(5), split2(coup_ref[0, 0]))

        @pl.when(fp1)
        def _():
            c = split2(coup_ref[0, 1])
            f_ref[0] += dot3(wt_of(3), c)
            f_ref[1] = dot3(wt_of(4), c)

        @pl.when(fm1)
        def _():
            c = split2(coup_ref[0, 2])
            f_ref[1] += dot3(wt_of(0), c)
            f_ref[2] = dot3(wt_of(1), c)
            f_ref[3] = dot3(wt_of(6), c)

        @pl.when(fm2)
        def _():
            c = split2(coup_ref[0, 3])
            f_ref[2] += dot3(wt_of(2), c)
            f_ref[3] = dot3(wt_of(6), c)

        y = [split2(a_part(i) - f_ref[i]) for i in range(3)]
        r_id = lax.broadcasted_iota(jnp.int32, (size, cols), 0)
        c_id = lax.broadcasted_iota(jnp.int32, (size, cols), 1) + base
        diag = jnp.where(r_id == c_id, shift_ref[:, pl.ds(base, cols)], 0.0)
        schur_ref[0, 2] = (
            dot3(at_of(0), y[0]) + dot3(at_of(1), y[1]) + dot3(at_of(2), y[2])
        ) + diag

        @pl.when(fm1)
        def _():
            schur_ref[0, 1] = coup_ref[0, 2]

        @pl.when(jnp.logical_not(fm1))
        def _():
            schur_ref[0, 1] = dot3(q_of(0), y[1]) + dot3(q_of(1), y[2])

            @pl.when(fm2)
            def _():
                schur_ref[0, 1] -= dot3(q_of(2), split2(f_ref[3]))

        @pl.when(fm2)
        def _():
            schur_ref[0, 0] = coup_ref[0, 3]

        @pl.when(jnp.logical_not(fm2))
        def _():
            schur_ref[0, 0] = dot3(q_of(2), y[2])

            @pl.when(fm1)
            def _():
                schur_ref[0, 0] -= dot3(q_of(0), split2(f_ref[3]))


def last(flags, recv, ath, atl, q, shift, l, w1, w2, others):
    size = shift.shape[1]
    slots = recv.shape[0]
    cols = 256
    whole = pl.BlockSpec(memory_space=pltpu.VMEM)
    return pl.pallas_call(
        last_kernel,
        grid=(size // cols,),
        in_specs=[pl.BlockSpec(memory_space=pltpu.SMEM)] + [whole] * 15,
        out_specs=(
            pl.BlockSpec((1, 3, size, cols), lambda n: (0, 0, 0, n)),
            pl.BlockSpec((1, 4, size, cols), lambda n: (0, 0, 0, n)),
        ),
        out_shape=(
            jax.ShapeDtypeStruct((1, 3, size, size), F32),
            jax.ShapeDtypeStruct((1, 4, size, size), F32),
        ),
        scratch_shapes=[
            pltpu.VMEM((size, 3 * slots), BF16),
            pltpu.VMEM((size, 3 * slots), BF16),
            pltpu.VMEM((6, size, slots), BF16),
            pltpu.VMEM((6, size, slots), BF16),
            pltpu.VMEM((7, slots, size), BF16),
            pltpu.VMEM((7, slots, size), BF16),
            pltpu.VMEM((4, slots, cols), F32),
        ],
        compiler_params=pltpu.CompilerParams(vmem_limit_bytes=62 * 2**20),
        name="last",
    )(flags, recv, ath, atl, q, shift, l, w1, w2, *others)


def passed_along(value, steps):
    count = lax.axis_size(AXES)
    pairs = [(source, (source + steps) % count) for source in range(count)]
    return lax.ppermute(value, AXES, pairs)


def exchange(payload):
    count = lax.axis_size(AXES)
    wide = payload.shape[1]
    got = lax.all_to_all(
        payload.reshape(count, -1, wide), AXES, split_axis=0, concat_axis=0, tiled=True
    )
    return got.reshape(payload.shape)


def local(strips, index, shift, flags):
    count = lax.axis_size(AXES)
    own = lax.axis_index(AXES)
    first, second = bucket(strips, index, flags)
    recv = exchange(first)
    l, w0, w1, w2, ath, atl = chol(recv, shift)
    q = exchange(second)
    near = jnp.take(flags, (own + jnp.arange(-2, 3)) % count)
    m1w0 = passed_along(w0, 1)
    m1w1 = passed_along(w1, 1)
    p1w2 = passed_along(w2, -1)
    p1w1 = passed_along(w1, -1)
    m2w0 = passed_along(m1w0, 1)
    p2w2 = passed_along(p1w2, -1)
    e = passed_along(jnp.where(near[2] > 0, w2, m1w1), 1)
    others = (m1w0, m1w1, m2w0, p1w1, p1w2, p2w2, e)
    return last(near, recv, ath, atl, q, shift, l, w1, w2, others)


def solution(mesh):
    in_specs = (P(AXES, None, None), P(AXES, None), P(AXES, None), P())
    out_specs = (P(AXES, None, None, None), P(AXES, None, None, None))
    return jax.shard_map(local, mesh=mesh, in_specs=in_specs, out_specs=out_specs, check_vma=False)
```

```python
import jax
import jax.numpy as jnp
from jax import lax
from jax.experimental import pallas as pl
from jax.experimental.pallas import tpu as pltpu
from jax.sharding import PartitionSpec as P

F32 = jnp.float32
BF16 = jnp.bfloat16
AXES = ("gx", "gy")


def split2(x):
    hi = x.astype(BF16)
    lo = (x - hi.astype(F32)).astype(BF16)
    return hi, lo


def dg(x, y, dims=((1,), (0,))):
    return lax.dot_general(x, y, (dims, ((), ())), preferred_element_type=F32)


def dot3(x, y, dims=((1,), (0,))):
    return dg(x[0], y[0], dims) + (dg(x[0], y[1], dims) + dg(x[1], y[0], dims))


def pieces_of(strips_ref):
    pieces = []
    for i in range(3):
        x = strips_ref[i]
        hi = x.astype(BF16)
        rest = x - hi.astype(F32)
        mid = rest.astype(BF16)
        low = (rest - mid.astype(F32)).astype(BF16)
        pieces.append((hi, mid, low))
    return pieces


def hits_of(row, slot):
    n = row.shape[1]
    r_id = lax.broadcasted_iota(jnp.int32, (n, n), 0)
    c_id = lax.broadcasted_iota(jnp.int32, (n, n), 1)
    wide = jnp.broadcast_to(row, (n, n))
    same = jnp.where((wide.T == wide) & (r_id < c_id), 1, 0)
    within = jnp.sum(same, axis=0, keepdims=True)
    return [(within == slot) & (((row + shift) & (n - 1)) == r_id) for shift in range(4)]


def as_mask(cond):
    return jnp.where(cond, 1.0, 0.0).astype(BF16)


def pick(select, piece):
    hi, mid, low = piece
    return dg(select, hi) + (dg(select, mid) + dg(select, low))


def first_kernel(strips_ref, row_ref, out_ref):
    width = strips_ref.shape[2]
    pieces = pieces_of(strips_ref)
    for slot in range(2):
        hit = hits_of(row_ref[...], slot)
        for i in range(3):
            out_ref[:, slot, i * width : (i + 1) * width] = pick(as_mask(hit[i]), pieces[i])


def second_kernel(strips_ref, row_ref, flag_ref, out_ref):
    width = strips_ref.shape[2]
    n = row_ref.shape[1]
    pieces = pieces_of(strips_ref)
    flags = flag_ref[...]
    r_id = lax.broadcasted_iota(jnp.int32, (n, n), 0)
    c_id = lax.broadcasted_iota(jnp.int32, (n, n), 1)

    def flag_before(step):
        chosen = c_id == ((r_id + (n - step)) & (n - 1))
        return jnp.sum(jnp.where(chosen, flags, 0), axis=1, keepdims=True) > 0

    one_before = flag_before(1)
    two_before = flag_before(2)
    for slot in range(2):
        hit = hits_of(row_ref[...], slot)
        out_ref[:, slot, 0:width] = pick(as_mask(hit[1] & ~one_before), pieces[0]) + pick(
            as_mask(hit[3] & one_before), pieces[1]
        )
        out_ref[:, slot, width : 2 * width] = pick(as_mask(hit[2]), pieces[1])
        out_ref[:, slot, 2 * width : 3 * width] = pick(
            as_mask(hit[2] & ~two_before), pieces[0]
        ) + pick(as_mask(hit[3] & two_before), pieces[2])


def bucket(kernel, name, *args):
    n, wide = args[0].shape[1], 3 * args[0].shape[2]
    return pl.pallas_call(
        kernel,
        out_shape=jax.ShapeDtypeStruct((n, 2, wide), F32),
        cost_estimate=pl.CostEstimate(
            flops=10 * n * n * wide, bytes_accessed=12 * n * wide, transcendentals=0
        ),
        name=name,
    )(*args)


def chol_block(a):
    n = a.shape[0]
    groups = n // 8
    sub = lax.broadcasted_iota(jnp.int32, (8, n), 0)
    lane = lax.broadcasted_iota(jnp.int32, (8, n), 1)
    left = [a[8 * v : 8 * v + 8, :] for v in range(groups)]
    right = [jnp.where(lane == sub + 8 * v, 1.0, 0.0).astype(F32) for v in range(groups)]

    def lanes_of(x, k):
        return [jnp.broadcast_to(x[:, 8 * k + i : 8 * k + i + 1], (8, n)) for i in range(8)]

    def sub_of(x, i):
        return jnp.broadcast_to(x[i : i + 1, :], (8, n))

    for k in range(groups):
        c = lanes_of(left[k], k)
        u, v_in = left[k], right[k]
        scale, row_u, row_v, row_c = [], [], [], []
        for i in range(8):
            inv = lax.rsqrt(sub_of(c[i], i))
            ru = sub_of(u, i) * inv
            rv = sub_of(v_in, i) * inv
            rc = [None] * 8
            m = jnp.where(sub > i, c[i] * inv, 0.0)
            for j in range(i + 1, 8):
                rc[j] = sub_of(c[j], i) * inv
                c[j] = c[j] - m * rc[j]
            u = jnp.where(sub == i, ru, u - m * ru)
            v_in = jnp.where(sub == i, rv, v_in - m * rv)
            scale.append(inv)
            row_u.append(ru)
            row_v.append(rv)
            row_c.append(rc)
        left[k], right[k] = u, v_in
        for g in range(k + 1, groups):
            c = lanes_of(left[g], k)
            x, y = left[g], right[g]
            for i in range(8):
                m = c[i] * scale[i]
                for j in range(i + 1, 8):
                    c[j] = c[j] - m * row_c[i][j]
                x = x - m * row_u[i]
                y = y - m * row_v[i]
            left[g], right[g] = x, y
    upper = jnp.concatenate(left, axis=0)
    r_id = lax.broadcasted_iota(jnp.int32, (n, n), 0)
    c_id = lax.broadcasted_iota(jnp.int32, (n, n), 1)
    return jnp.where(c_id >= r_id, upper, 0.0), jnp.concatenate(right, axis=0)


MESH = pl.DeviceIdType.MESH


def chol_kernel(
    recv_ref, shift_ref, flag_ref,
    l_ref, w1_ref, w2_ref, ath_ref, atl_ref, c_ref, f_ref,
    m1w0_ref, m1w1_ref, m2w0_ref, p1w1_ref, p1w2_ref, p2w2_ref, gx_ref, gy_ref,
    m_ref, x_ref, w0_ref, ah_ref, al_ref, outx_ref, outy_ref, gram_ref,
    send_sem, recv_sem, small_send, small_recv,
):
    size = shift_ref.shape[1]
    slots = w0_ref.shape[1]
    half = slots // 2
    nb = 128
    count = size // nb
    rows_y = lax.axis_size("gy")
    total_dev = lax.axis_size("gx") * rows_y
    own = lax.axis_index("gx") * rows_y + lax.axis_index("gy")
    up = lax.rem(own + 1, total_dev)
    down = lax.rem(own + total_dev - 1, total_dev)
    up_id = (lax.div(up, rows_y), lax.rem(up, rows_y))
    down_id = (lax.div(down, rows_y), lax.rem(down, rows_y))

    barrier = pltpu.get_barrier_semaphore()
    for there in (up_id, down_id):
        pl.semaphore_signal(barrier, inc=1, device_id=there, device_id_type=MESH)

    def rows(k):
        return pl.ds(pl.multiple_of(k * nb, nb), nb)

    def copy(which, k):
        source, target, there = (
            (w0_ref, m1w0_ref, up_id),
            (w1_ref, m1w1_ref, up_id),
            (m1w0_ref, m2w0_ref, up_id),
            (w1_ref, p1w1_ref, down_id),
            (w2_ref, p1w2_ref, down_id),
            (p1w2_ref, p2w2_ref, down_id),
        )[which]
        return pltpu.make_async_remote_copy(
            src_ref=source.at[rows(k), :],
            dst_ref=target.at[rows(k), :],
            send_sem=send_sem.at[which, k],
            recv_sem=recv_sem.at[which, k],
            device_id=there,
            device_id_type=MESH,
        )

    def small(which):
        source, target = ((outx_ref, gx_ref), (outy_ref, gy_ref))[which]
        return pltpu.make_async_remote_copy(
            src_ref=source,
            dst_ref=target,
            send_sem=small_send.at[which],
            recv_sem=small_recv.at[which],
            device_id=up_id,
            device_id_type=MESH,
        )

    def relay(k):
        copy(0, k).wait_recv()
        copy(2, k).start()
        copy(4, k).wait_recv()
        copy(5, k).start()

    l_ref[...] = jnp.zeros_like(l_ref)
    f_ref[...] = jnp.zeros_like(f_ref)
    gram_ref[...] = jnp.zeros_like(gram_ref)
    for i in range(3):
        for s in range(2):
            x = recv_ref[:, s, i * size : (i + 1) * size]
            hi, lo = split2(x)
            ah_ref[i, s * half : (s + 1) * half, :] = hi
            al_ref[i, s * half : (s + 1) * half, :] = lo
            at = x.T
            begin = i * slots + s * half
            m_ref[:, size + begin : size + begin + half] = at
            hi, lo = split2(at)
            ath_ref[:, begin : begin + half] = hi
            atl_ref[:, begin : begin + half] = lo
    for blk in range(0, size, 256):
        total = None
        for i in range(3):
            a = (ah_ref[i, :, blk : blk + 256], al_ref[i, :, blk : blk + 256])
            t = (ath_ref[:, i * slots : (i + 1) * slots], atl_ref[:, i * slots : (i + 1) * slots])
            add = dot3(t, a)
            total = add if total is None else total + add
        r_id = lax.broadcasted_iota(jnp.int32, (size, 256), 0)
        c_id = lax.broadcasted_iota(jnp.int32, (size, 256), 1) + blk
        m_ref[:, blk : blk + 256] = total + jnp.where(
            r_id == c_id, shift_ref[:, blk : blk + 256], 0.0
        )
    pl.semaphore_wait(barrier, 2)

    w_refs = (w0_ref, w1_ref, w2_ref)

    def step(k, carry):
        at = pl.multiple_of(k * nb, nb)
        upper, inverse = chol_block(m_ref[pl.ds(at, nb), pl.ds(at, nb)])
        l_ref[pl.ds(at, nb), pl.ds(at, nb)] = upper.T
        inv = split2(inverse)
        for blk in range(0, 2 * size, 256):
            x_ref[:, blk : blk + 256] = dot3(inv, split2(m_ref[pl.ds(at, nb), blk : blk + 256]))
        for i in range(3):
            w_refs[i][pl.ds(at, nb), :] = x_ref[:, size + i * slots : size + (i + 1) * slots]

        def trail(r, inner):
            to = pl.multiple_of(r * nb, nb)
            low = x_ref[:, pl.ds(to, nb)].T
            l_ref[pl.ds(to, nb), pl.ds(at, nb)] = low
            low = split2(low)
            for blk in range(0, 2 * size, 256):
                m_ref[pl.ds(to, nb), blk : blk + 256] -= dot3(
                    low, split2(x_ref[:, blk : blk + 256])
                )
            return inner

        lax.fori_loop(k + 1, count, trail, carry)
        wt = split2(x_ref[:, size + 2 * slots : size + 3 * slots].T)
        for j in range(2):
            gram_ref[j] += dot3(wt, split2(x_ref[:, size + j * slots : size + (j + 1) * slots]))
        for which in (0, 4, 1, 3):
            copy(which, k).start()

        @pl.when(k >= 2)
        def _():
            relay(k - 2)

        return carry

    lax.fori_loop(0, count, step, 0)

    flag = [flag_ref[i : i + 1, 0:1] for i in range(5)]
    outx_ref[...] = gram_ref[0] * flag[2]

    def a_of(i):
        return ah_ref[i], al_ref[i]

    def near(k, carry):
        copy(1, k).wait_recv()
        copy(3, k).wait_recv()

        @pl.when(k >= count - 2)
        def _():
            relay(k)

        p1w1, p1w2 = p1w1_ref[rows(k), :], p1w2_ref[rows(k), :]
        m1w0, m1w1 = m1w0_ref[rows(k), :], m1w1_ref[rows(k), :]
        c = dot3(split2(p1w1), a_of(0)) + dot3(split2(p1w2), a_of(1))
        c_ref[1, rows(k), :] = c
        c = split2(c * flag[3])
        f_ref[0] += dot3(split2(p1w1.T), c)
        f_ref[1] += dot3(split2(p1w2.T), c)
        m1w0s = split2(m1w0)
        c = dot3(m1w0s, a_of(1)) + dot3(split2(m1w1), a_of(2))
        c_ref[2, rows(k), :] = c
        c = split2(c * flag[1])
        w1t = split2(m1w1.T)
        f_ref[1] += dot3(split2(m1w0.T), c)
        f_ref[2] += dot3(w1t, c)
        gram_ref[2] += dot3(w1t, m1w0s)

        @pl.when(k == 0)
        def _():
            small(0).start()

        return carry

    lax.fori_loop(0, count, near, 0)
    outy_ref[...] = gram_ref[1] * flag[2] + gram_ref[2] * (1.0 - flag[2])

    def far(k, carry):
        copy(2, k).wait_recv()
        copy(5, k).wait_recv()
        w = p2w2_ref[rows(k), :]
        c = dot3(split2(w), a_of(0))
        c_ref[0, rows(k), :] = c
        f_ref[0] += dot3(split2(w.T), split2(c * flag[4]))
        w = m2w0_ref[rows(k), :]
        c = dot3(split2(w), a_of(2))
        c_ref[3, rows(k), :] = c
        f_ref[2] += dot3(split2(w.T), split2(c * flag[0]))

        @pl.when(k == 0)
        def _():
            small(1).start()

        return carry

    lax.fori_loop(0, count, far, 0)
    for which in range(2):
        small(which).wait_recv()
    f_ref[3] = dot3(split2(gx_ref[...]), a_of(1)) + dot3(split2(gy_ref[...]), a_of(2))
    for which in range(2):
        small(which).wait_send()

    def drain(k, carry):
        for which in range(6):
            copy(which, k).wait_send()
        return carry

    lax.fori_loop(0, count, drain, 0)


def chol(recv, shift, flags):
    size = shift.shape[1]
    slots = 2 * recv.shape[0]
    w = jax.ShapeDtypeStruct((size, slots), F32)
    low = jax.ShapeDtypeStruct((size, 3 * slots), BF16)
    square = jax.ShapeDtypeStruct((slots, slots), F32)
    count = size // 128
    return pl.pallas_call(
        chol_kernel,
        out_shape=(
            jax.ShapeDtypeStruct((size, size), F32), w, w, low, low,
            jax.ShapeDtypeStruct((4, size, size), F32),
            jax.ShapeDtypeStruct((4, slots, size), F32),
        ),
        scratch_shapes=[pltpu.VMEM((size, slots), F32)] * 6
        + [pltpu.VMEM((slots, slots), F32)] * 2
        + [
            pltpu.VMEM((size, size + 3 * slots), F32),
            pltpu.VMEM((128, size + 3 * slots), F32),
            pltpu.VMEM((size, slots), F32),
            pltpu.VMEM((3, slots, size), BF16),
            pltpu.VMEM((3, slots, size), BF16),
            pltpu.VMEM((slots, slots), F32),
            pltpu.VMEM((slots, slots), F32),
            pltpu.VMEM((3, slots, slots), F32),
            pltpu.SemaphoreType.DMA((6, count)),
            pltpu.SemaphoreType.DMA((6, count)),
            pltpu.SemaphoreType.DMA((2,)),
            pltpu.SemaphoreType.DMA((2,)),
        ],
        compiler_params=pltpu.CompilerParams(
            vmem_limit_bytes=56 * 2**20, collective_id=0, has_side_effects=True
        ),
        cost_estimate=pl.CostEstimate(
            flops=30 * size * size * size, bytes_accessed=30 * size * size, transcendentals=0
        ),
        name="chol",
    )(recv, shift, flags)


def last_kernel(
    flag_ref, recv_ref, ath_ref, atl_ref, q_ref, shift_ref, l_ref, w1_ref, w2_ref, c_ref, f_ref,
    schur_ref, coup_ref, qh_ref, ql_ref, sem,
):
    step = pl.program_id(0)
    size = shift_ref.shape[1]
    slots = w1_ref.shape[1]
    half = slots // 2
    cols = schur_ref.shape[3]
    fm2, fm1, own = [flag_ref[i] > 0 for i in range(3)]
    out = pltpu.make_async_copy(c_ref, coup_ref.at[0], sem)

    @pl.when(step == 0)
    def _():
        out.start()
        for i in range(3):
            for s in range(2):
                begin = i * slots + s * half
                hi, lo = split2(q_ref[:, s, i * size : (i + 1) * size].T)
                qh_ref[:, begin : begin + half] = hi
                ql_ref[:, begin : begin + half] = lo

    base = pl.multiple_of(step * cols, cols)
    span = pl.ds(base, cols)

    def at_of(i):
        return ath_ref[:, i * slots : (i + 1) * slots], atl_ref[:, i * slots : (i + 1) * slots]

    def q_of(i):
        return qh_ref[:, i * slots : (i + 1) * slots], ql_ref[:, i * slots : (i + 1) * slots]

    @pl.when(own)
    def _():
        w1 = split2(w1_ref[span, :])
        w2 = split2(w2_ref[span, :])
        over = ((1,), (1,))
        schur_ref[0, 0] = dot3(q_of(2), w2, over)
        schur_ref[0, 1] = dot3(q_of(0), w1, over) + dot3(q_of(1), w2, over)
        schur_ref[0, 2] = l_ref[:, span]

    @pl.when(jnp.logical_not(own))
    def _():
        y = []
        for i in range(3):
            lanes = pl.ds(pl.multiple_of(i * size + base, cols), cols)
            a = jnp.concatenate([recv_ref[:, 0, lanes], recv_ref[:, 1, lanes]], axis=0)
            y.append(split2(a - f_ref[i, :, span]))
        r_id = lax.broadcasted_iota(jnp.int32, (size, cols), 0)
        c_id = lax.broadcasted_iota(jnp.int32, (size, cols), 1) + base
        diag = jnp.where(r_id == c_id, shift_ref[:, span], 0.0)
        schur_ref[0, 2] = (
            dot3(at_of(0), y[0]) + dot3(at_of(1), y[1]) + dot3(at_of(2), y[2])
        ) + diag

        @pl.when(fm1)
        def _():
            schur_ref[0, 1] = c_ref[2, :, span]

        @pl.when(jnp.logical_not(fm1))
        def _():
            schur_ref[0, 1] = dot3(q_of(0), y[1]) + dot3(q_of(1), y[2])

            @pl.when(fm2)
            def _():
                schur_ref[0, 1] -= dot3(q_of(2), split2(f_ref[3, :, span]))

        @pl.when(fm2)
        def _():
            schur_ref[0, 0] = c_ref[3, :, span]

        @pl.when(jnp.logical_not(fm2))
        def _():
            schur_ref[0, 0] = dot3(q_of(2), y[2])

            @pl.when(fm1)
            def _():
                schur_ref[0, 0] -= dot3(q_of(0), split2(f_ref[3, :, span]))

    @pl.when(step == pl.num_programs(0) - 1)
    def _():
        out.wait()


def last(flags, recv, q, shift, l, w1, w2, ath, atl, c, f):
    size = shift.shape[1]
    slots = w1.shape[1]
    cols = 256
    whole = pl.BlockSpec(memory_space=pltpu.VMEM)
    return pl.pallas_call(
        last_kernel,
        grid=(size // cols,),
        in_specs=[pl.BlockSpec(memory_space=pltpu.SMEM)] + [whole] * 10,
        out_specs=(
            pl.BlockSpec((1, 3, size, cols), lambda n: (0, 0, 0, n)),
            pl.BlockSpec(memory_space=pl.ANY),
        ),
        out_shape=(
            jax.ShapeDtypeStruct((1, 3, size, size), F32),
            jax.ShapeDtypeStruct((1, 4, size, size), F32),
        ),
        scratch_shapes=[
            pltpu.VMEM((size, 3 * slots), BF16),
            pltpu.VMEM((size, 3 * slots), BF16),
            pltpu.SemaphoreType.DMA,
        ],
        compiler_params=pltpu.CompilerParams(vmem_limit_bytes=44 * 2**20),
        name="last",
    )(flags, recv, ath, atl, q, shift, l, w1, w2, c, f)


def exchange(payload):
    return lax.all_to_all(payload, AXES, split_axis=0, concat_axis=0, tiled=True)


def local(strips, index, shift, flags):
    count = lax.axis_size(AXES)
    own = lax.axis_index(AXES)
    strips = jnp.transpose(strips, (1, 0, 2))
    index = index.reshape(1, -1)
    first = bucket(first_kernel, "first", strips, index)
    recv = exchange(first)
    second = bucket(second_kernel, "second", strips, index, flags.reshape(1, -1))
    near = jnp.take(flags, (own + jnp.arange(-2, 6)) % count)
    wide = jnp.broadcast_to(near.astype(F32)[:, None], (8, 128))
    parts = chol(recv, shift, wide)
    q = exchange(second)
    return last(near, recv, q, shift, *parts)


def solution(mesh):
    in_specs = (P(AXES, None, None), P(AXES, None), P(AXES, None), P())
    out_specs = (P(AXES, None, None, None), P(AXES, None, None, None))
    return jax.shard_map(local, mesh=mesh, in_specs=in_specs, out_specs=out_specs, check_vma=False)
```

```python
import jax
import jax.numpy as jnp
from jax import lax
from jax.experimental import pallas as pl
from jax.experimental.pallas import tpu as pltpu
from jax.sharding import PartitionSpec as P

F32 = jnp.float32
BF16 = jnp.bfloat16
AXES = ("gx", "gy")


def split2(x):
    hi = x.astype(BF16)
    lo = (x - hi.astype(F32)).astype(BF16)
    return hi, lo


def dg(x, y, dims=((1,), (0,))):
    return lax.dot_general(x, y, (dims, ((), ())), preferred_element_type=F32)


def dot3(x, y, dims=((1,), (0,))):
    return dg(x[0], y[0], dims) + (dg(x[0], y[1], dims) + dg(x[1], y[0], dims))


def dot3_short(x, y):
    both = dg(jnp.concatenate(x, axis=1), jnp.concatenate([y[0], y[0]], axis=0))
    return both + dg(x[0], y[1])


def pieces_of(strips_ref):
    pieces = []
    for i in range(3):
        x = strips_ref[i]
        hi = x.astype(BF16)
        rest = x - hi.astype(F32)
        mid = rest.astype(BF16)
        low = (rest - mid.astype(F32)).astype(BF16)
        pieces.append((hi, mid, low))
    return pieces


def hits_of(row, slot):
    n = row.shape[1]
    r_id = lax.broadcasted_iota(jnp.int32, (n, n), 0)
    c_id = lax.broadcasted_iota(jnp.int32, (n, n), 1)
    wide = jnp.broadcast_to(row, (n, n))
    same = jnp.where((wide.T == wide) & (r_id < c_id), 1, 0)
    within = jnp.sum(same, axis=0, keepdims=True)
    return [(within == slot) & (((row + shift) & (n - 1)) == r_id) for shift in range(4)]


def as_mask(cond):
    return jnp.where(cond, 1.0, 0.0).astype(BF16)


def pick(select, piece):
    hi, mid, low = piece
    return dg(select, hi) + (dg(select, mid) + dg(select, low))


def first_kernel(strips_ref, row_ref, out_ref):
    width = strips_ref.shape[2]
    pieces = pieces_of(strips_ref)
    for slot in range(2):
        hit = hits_of(row_ref[...], slot)
        for i in range(3):
            out_ref[:, slot, i * width : (i + 1) * width] = pick(as_mask(hit[i]), pieces[i])


def second_kernel(strips_ref, row_ref, flag_ref, out_ref):
    width = strips_ref.shape[2]
    n = row_ref.shape[1]
    pieces = pieces_of(strips_ref)
    flags = flag_ref[...]
    r_id = lax.broadcasted_iota(jnp.int32, (n, n), 0)
    c_id = lax.broadcasted_iota(jnp.int32, (n, n), 1)

    def flag_before(step):
        chosen = c_id == ((r_id + (n - step)) & (n - 1))
        return jnp.sum(jnp.where(chosen, flags, 0), axis=1, keepdims=True) > 0

    one_before = flag_before(1)
    two_before = flag_before(2)
    for slot in range(2):
        hit = hits_of(row_ref[...], slot)
        out_ref[:, slot, 0:width] = pick(as_mask(hit[1] & ~one_before), pieces[0]) + pick(
            as_mask(hit[3] & one_before), pieces[1]
        )
        out_ref[:, slot, width : 2 * width] = pick(as_mask(hit[2]), pieces[1])
        out_ref[:, slot, 2 * width : 3 * width] = pick(
            as_mask(hit[2] & ~two_before), pieces[0]
        ) + pick(as_mask(hit[3] & two_before), pieces[2])


def bucket(kernel, name, *args):
    n, wide = args[0].shape[1], 3 * args[0].shape[2]
    return pl.pallas_call(
        kernel,
        out_shape=jax.ShapeDtypeStruct((n, 2, wide), F32),
        cost_estimate=pl.CostEstimate(
            flops=10 * n * n * wide, bytes_accessed=12 * n * wide, transcendentals=0
        ),
        name=name,
    )(*args)


def chol_block(a):
    n = a.shape[0]
    groups = n // 8
    sub = lax.broadcasted_iota(jnp.int32, (8, n), 0)
    lane = lax.broadcasted_iota(jnp.int32, (8, n), 1)
    left = [a[8 * v : 8 * v + 8, :] for v in range(groups)]
    right = [jnp.where(lane == sub + 8 * v, 1.0, 0.0).astype(F32) for v in range(groups)]

    def lanes_of(x, k):
        return [jnp.broadcast_to(x[:, 8 * k + i : 8 * k + i + 1], (8, n)) for i in range(8)]

    def sub_of(x, i):
        return jnp.broadcast_to(x[i : i + 1, :], (8, n))

    for k in range(groups):
        c = lanes_of(left[k], k)
        u, v_in = left[k], right[k]
        scale, row_u, row_v, row_c = [], [], [], []
        for i in range(8):
            inv = lax.rsqrt(sub_of(c[i], i))
            ru = sub_of(u, i) * inv
            rv = sub_of(v_in, i) * inv
            rc = [None] * 8
            m = jnp.where(sub > i, c[i] * inv, 0.0)
            for j in range(i + 1, 8):
                rc[j] = sub_of(c[j], i) * inv
                c[j] = c[j] - m * rc[j]
            u = jnp.where(sub == i, ru, u - m * ru)
            v_in = jnp.where(sub == i, rv, v_in - m * rv)
            scale.append(inv)
            row_u.append(ru)
            row_v.append(rv)
            row_c.append(rc)
        left[k], right[k] = u, v_in
        for g in range(k + 1, groups):
            c = lanes_of(left[g], k)
            x, y = left[g], right[g]
            for i in range(8):
                m = c[i] * scale[i]
                for j in range(i + 1, 8):
                    c[j] = c[j] - m * row_c[i][j]
                x = x - m * row_u[i]
                y = y - m * row_v[i]
            left[g], right[g] = x, y
    upper = jnp.concatenate(left, axis=0)
    r_id = lax.broadcasted_iota(jnp.int32, (n, n), 0)
    c_id = lax.broadcasted_iota(jnp.int32, (n, n), 1)
    return jnp.where(c_id >= r_id, upper, 0.0), jnp.concatenate(right, axis=0)


MESH = pl.DeviceIdType.MESH


def chol_kernel(
    recv_ref, shift_ref, flag_ref,
    l_ref, w1_ref, w2_ref, ath_ref, atl_ref, cout_ref, f_ref,
    c_ref,
    m1w0_ref, m1w1_ref, m2w0_ref, p1w1_ref, p1w2_ref, p2w2_ref, gx_ref, gy_ref,
    m_ref, x_ref, w0_ref, ah_ref, al_ref, outx_ref, outy_ref, gram_ref,
    send_sem, recv_sem, small_send, small_recv, c_sem,
):
    size = shift_ref.shape[1]
    slots = w0_ref.shape[1]
    half = slots // 2
    nb = 128
    count = size // nb
    rows_y = lax.axis_size("gy")
    total_dev = lax.axis_size("gx") * rows_y
    own = lax.axis_index("gx") * rows_y + lax.axis_index("gy")
    up = lax.rem(own + 1, total_dev)
    down = lax.rem(own + total_dev - 1, total_dev)
    up_id = (lax.div(up, rows_y), lax.rem(up, rows_y))
    down_id = (lax.div(down, rows_y), lax.rem(down, rows_y))

    barrier = pltpu.get_barrier_semaphore()
    for there in (up_id, down_id):
        pl.semaphore_signal(barrier, inc=1, device_id=there, device_id_type=MESH)

    def rows(k):
        return pl.ds(pl.multiple_of(k * nb, nb), nb)

    def copy(which, k):
        source, target, there = (
            (w0_ref, m1w0_ref, up_id),
            (w1_ref, m1w1_ref, up_id),
            (m1w0_ref, m2w0_ref, up_id),
            (w1_ref, p1w1_ref, down_id),
            (w2_ref, p1w2_ref, down_id),
            (p1w2_ref, p2w2_ref, down_id),
        )[which]
        return pltpu.make_async_remote_copy(
            src_ref=source.at[rows(k), :],
            dst_ref=target.at[rows(k), :],
            send_sem=send_sem.at[which, k],
            recv_sem=recv_sem.at[which, k],
            device_id=there,
            device_id_type=MESH,
        )

    def small(which):
        source, target = ((outx_ref, gx_ref), (outy_ref, gy_ref))[which]
        return pltpu.make_async_remote_copy(
            src_ref=source,
            dst_ref=target,
            send_sem=small_send.at[which],
            recv_sem=small_recv.at[which],
            device_id=up_id,
            device_id_type=MESH,
        )

    def relay(k):
        copy(0, k).wait_recv()
        copy(2, k).start()
        copy(4, k).wait_recv()
        copy(5, k).start()

    l_ref[...] = jnp.zeros_like(l_ref)
    f_ref[...] = jnp.zeros_like(f_ref)
    gram_ref[...] = jnp.zeros_like(gram_ref)
    for i in range(3):
        for s in range(2):
            x = recv_ref[:, s, i * size : (i + 1) * size]
            hi, lo = split2(x)
            ah_ref[i, s * half : (s + 1) * half, :] = hi
            al_ref[i, s * half : (s + 1) * half, :] = lo
            at = x.T
            begin = i * slots + s * half
            m_ref[:, size + begin : size + begin + half] = at
            hi, lo = split2(at)
            ath_ref[:, begin : begin + half] = hi
            atl_ref[:, begin : begin + half] = lo
    for blk in range(0, size, 256):
        total = None
        for i in range(3):
            a = (ah_ref[i, :, blk : blk + 256], al_ref[i, :, blk : blk + 256])
            here = slice(i * slots, (i + 1) * slots)
            t = (ath_ref[0 : blk + 256, here], atl_ref[0 : blk + 256, here])
            add = dot3(t, a)
            total = add if total is None else total + add
        r_id = lax.broadcasted_iota(jnp.int32, (blk + 256, 256), 0)
        c_id = lax.broadcasted_iota(jnp.int32, (blk + 256, 256), 1) + blk
        m_ref[0 : blk + 256, blk : blk + 256] = total + jnp.where(
            r_id == c_id, shift_ref[:, blk : blk + 256], 0.0
        )
    pl.semaphore_wait(barrier, 2)

    w_refs = (w0_ref, w1_ref, w2_ref)

    def step(k, carry):
        at = pl.multiple_of(k * nb, nb)
        upper, inverse = chol_block(m_ref[pl.ds(at, nb), pl.ds(at, nb)])
        l_ref[pl.ds(at, nb), pl.ds(at, nb)] = upper.T
        inv = split2(inverse)
        for blk in range(size, 2 * size, 256):
            x_ref[:, blk : blk + 256] = dot3_short(
                inv, split2(m_ref[pl.ds(at, nb), blk : blk + 256])
            )
        for blk in range(0, size, 256):

            @pl.when(blk + 256 > at + nb)
            def _(blk=blk):
                x_ref[:, blk : blk + 256] = dot3_short(
                    inv, split2(m_ref[pl.ds(at, nb), blk : blk + 256])
                )
        for i in range(3):
            w_refs[i][pl.ds(at, nb), :] = x_ref[:, size + i * slots : size + (i + 1) * slots]

        def trail(r, inner):
            to = pl.multiple_of(r * nb, nb)
            low = x_ref[:, pl.ds(to, nb)].T
            l_ref[pl.ds(to, nb), pl.ds(at, nb)] = low
            low = split2(low)
            for blk in range(size, 2 * size, 256):
                m_ref[pl.ds(to, nb), blk : blk + 256] -= dot3_short(
                    low, split2(x_ref[:, blk : blk + 256])
                )
            for blk in range(0, size, 256):

                @pl.when(blk + 256 > to)
                def _(blk=blk):
                    m_ref[pl.ds(to, nb), blk : blk + 256] -= dot3_short(
                        low, split2(x_ref[:, blk : blk + 256])
                    )

            return inner

        lax.fori_loop(k + 1, count, trail, carry)
        wt = split2(x_ref[:, size + 2 * slots : size + 3 * slots].T)
        for j in range(2):
            gram_ref[j] += dot3_short(
                wt, split2(x_ref[:, size + j * slots : size + (j + 1) * slots])
            )
        for which in (0, 4, 1, 3):
            copy(which, k).start()

        @pl.when(k >= 2)
        def _():
            relay(k - 2)

        return carry

    lax.fori_loop(0, count, step, 0)

    flag = [flag_ref[i : i + 1, 0:1] for i in range(5)]
    outx_ref[...] = gram_ref[0] * flag[2]

    def a_of(i):
        return ah_ref[i], al_ref[i]

    def out_copy(which, k):
        return pltpu.make_async_copy(
            c_ref.at[which, wide(k), :], cout_ref.at[which, wide(k), :], c_sem.at[which, k]
        )

    def wide(k):
        return pl.ds(pl.multiple_of(k * 2 * nb, 2 * nb), 2 * nb)

    def near(k, carry):
        for part in range(2):
            copy(1, 2 * k + part).wait_recv()
            copy(3, 2 * k + part).wait_recv()

        @pl.when(k >= 1)
        def _():
            relay(k + 3)

        p1w1, p1w2 = p1w1_ref[wide(k), :], p1w2_ref[wide(k), :]
        c = dot3(split2(p1w1), a_of(0)) + dot3(split2(p1w2), a_of(1))
        c_ref[1, wide(k), :] = c
        c = split2(c * flag[3])
        f_ref[0] += dot3(split2(p1w1.T), c)
        f_ref[1] += dot3(split2(p1w2.T), c)

        @pl.when(k == 0)
        def _():
            small(0).start()

        m1w0, m1w1 = m1w0_ref[wide(k), :], m1w1_ref[wide(k), :]
        m1w0s = split2(m1w0)
        c = dot3(m1w0s, a_of(1)) + dot3(split2(m1w1), a_of(2))
        c_ref[2, wide(k), :] = c
        c = split2(c * flag[1])
        w1t = split2(m1w1.T)
        f_ref[1] += dot3(split2(m1w0.T), c)
        f_ref[2] += dot3(w1t, c)
        gram_ref[2] += dot3(w1t, m1w0s)
        out_copy(1, k).start()
        out_copy(2, k).start()
        return carry

    lax.fori_loop(0, count // 2, near, 0)
    outy_ref[...] = gram_ref[1] * flag[2] + gram_ref[2] * (1.0 - flag[2])

    def far(k, carry):
        for part in range(2):
            copy(2, 2 * k + part).wait_recv()
            copy(5, 2 * k + part).wait_recv()
        w = p2w2_ref[wide(k), :]
        c = dot3(split2(w), a_of(0))
        c_ref[0, wide(k), :] = c
        f_ref[0] += dot3(split2(w.T), split2(c * flag[4]))

        @pl.when(k == 0)
        def _():
            small(1).start()

        w = m2w0_ref[wide(k), :]
        c = dot3(split2(w), a_of(2))
        c_ref[3, wide(k), :] = c
        f_ref[2] += dot3(split2(w.T), split2(c * flag[0]))
        out_copy(0, k).start()
        out_copy(3, k).start()
        return carry

    lax.fori_loop(0, count // 2, far, 0)
    for which in range(2):
        small(which).wait_recv()
    f_ref[3] = dot3(split2(gx_ref[...]), a_of(1)) + dot3(split2(gy_ref[...]), a_of(2))
    for which in range(2):
        small(which).wait_send()
    for which in range(4):
        for k in range(count // 2):
            out_copy(which, k).wait()

    def drain(k, carry):
        for which in range(6):
            copy(which, k).wait_send()
        return carry

    lax.fori_loop(0, count, drain, 0)


def chol(recv, shift, flags):
    size = shift.shape[1]
    slots = 2 * recv.shape[0]
    w = jax.ShapeDtypeStruct((size, slots), F32)
    low = jax.ShapeDtypeStruct((size, 3 * slots), BF16)
    square = jax.ShapeDtypeStruct((slots, slots), F32)
    count = size // 128
    whole = pl.BlockSpec(memory_space=pltpu.VMEM)
    return pl.pallas_call(
        chol_kernel,
        out_shape=(
            jax.ShapeDtypeStruct((size, size), F32), w, w, low, low,
            jax.ShapeDtypeStruct((4, size, size), F32),
            jax.ShapeDtypeStruct((4, slots, size), F32),
        ),
        out_specs=(whole,) * 5 + (pl.BlockSpec(memory_space=pl.ANY), whole),
        scratch_shapes=[pltpu.VMEM((4, size, size), F32)]
        + [pltpu.VMEM((size, slots), F32)] * 6
        + [pltpu.VMEM((slots, slots), F32)] * 2
        + [
            pltpu.VMEM((size, size + 3 * slots), F32),
            pltpu.VMEM((128, size + 3 * slots), F32),
            pltpu.VMEM((size, slots), F32),
            pltpu.VMEM((3, slots, size), BF16),
            pltpu.VMEM((3, slots, size), BF16),
            pltpu.VMEM((slots, slots), F32),
            pltpu.VMEM((slots, slots), F32),
            pltpu.VMEM((3, slots, slots), F32),
            pltpu.SemaphoreType.DMA((6, count)),
            pltpu.SemaphoreType.DMA((6, count)),
            pltpu.SemaphoreType.DMA((2,)),
            pltpu.SemaphoreType.DMA((2,)),
            pltpu.SemaphoreType.DMA((4, count // 2)),
        ],
        compiler_params=pltpu.CompilerParams(
            vmem_limit_bytes=60 * 2**20, collective_id=0, has_side_effects=True
        ),
        cost_estimate=pl.CostEstimate(
            flops=30 * size * size * size, bytes_accessed=30 * size * size, transcendentals=0
        ),
        name="chol",
    )(recv, shift, flags)


def last_kernel(
    flag_ref, recv_ref, ath_ref, atl_ref, qin_ref, shift_ref, lin_ref, w1_ref, w2_ref, cin_ref, f_ref,
    schur_ref, coup_ref, q_ref, l_ref, c_ref, qh_ref, ql_ref, sem, in_sem, out_sem,
):
    step = pl.program_id(0)
    size = shift_ref.shape[1]
    slots = w1_ref.shape[1]
    half = slots // 2
    cols = schur_ref.shape[3]
    fm2, fm1, own = [flag_ref[i] > 0 for i in range(3)]
    get_q = pltpu.make_async_copy(qin_ref, q_ref, sem.at[0])
    get_l = pltpu.make_async_copy(lin_ref, l_ref, sem.at[1])
    get_c = [pltpu.make_async_copy(cin_ref.at[i], c_ref.at[i], in_sem.at[i]) for i in range(4)]
    put_c = [pltpu.make_async_copy(c_ref.at[i], coup_ref.at[0, i], out_sem.at[i]) for i in range(4)]

    @pl.when(step == 0)
    def _():
        get_q.start()
        get_l.start()
        for i in (2, 3, 0, 1):
            get_c[i].start()

    base = pl.multiple_of(step * cols, cols)
    span = pl.ds(base, cols)

    def at_of(i):
        return ath_ref[:, i * slots : (i + 1) * slots], atl_ref[:, i * slots : (i + 1) * slots]

    def q_of(i):
        return qh_ref[:, i * slots : (i + 1) * slots], ql_ref[:, i * slots : (i + 1) * slots]

    def y_of(i):
        lanes = pl.ds(pl.multiple_of(i * size + base, cols), cols)
        a = jnp.concatenate([recv_ref[:, 0, lanes], recv_ref[:, 1, lanes]], axis=0)
        return split2(a - f_ref[i, :, span])

    @pl.when(jnp.logical_not(own))
    def _():
        r_id = lax.broadcasted_iota(jnp.int32, (size, cols), 0)
        c_id = lax.broadcasted_iota(jnp.int32, (size, cols), 1) + base
        diag = jnp.where(r_id == c_id, shift_ref[:, span], 0.0)
        schur_ref[0, 2] = (
            dot3(at_of(0), y_of(0)) + dot3(at_of(1), y_of(1)) + dot3(at_of(2), y_of(2))
        ) + diag

    @pl.when(step == 0)
    def _():
        get_q.wait()
        for i in range(3):
            for s in range(2):
                begin = i * slots + s * half
                hi, lo = split2(q_ref[:, s, i * size : (i + 1) * size].T)
                qh_ref[:, begin : begin + half] = hi
                ql_ref[:, begin : begin + half] = lo
        get_l.wait()
        for i in (2, 3, 0, 1):
            get_c[i].wait()
            put_c[i].start()

    @pl.when(own)
    def _():
        w1 = split2(w1_ref[span, :])
        w2 = split2(w2_ref[span, :])
        over = ((1,), (1,))
        schur_ref[0, 0] = dot3(q_of(2), w2, over)
        schur_ref[0, 1] = dot3(q_of(0), w1, over) + dot3(q_of(1), w2, over)
        schur_ref[0, 2] = l_ref[:, span]

    @pl.when(jnp.logical_not(own))
    def _():
        @pl.when(fm1)
        def _():
            schur_ref[0, 1] = c_ref[2, :, span]

        @pl.when(jnp.logical_not(fm1))
        def _():
            schur_ref[0, 1] = dot3(q_of(0), y_of(1)) + dot3(q_of(1), y_of(2))

            @pl.when(fm2)
            def _():
                schur_ref[0, 1] -= dot3(q_of(2), split2(f_ref[3, :, span]))

        @pl.when(fm2)
        def _():
            schur_ref[0, 0] = c_ref[3, :, span]

        @pl.when(jnp.logical_not(fm2))
        def _():
            schur_ref[0, 0] = dot3(q_of(2), y_of(2))

            @pl.when(fm1)
            def _():
                schur_ref[0, 0] -= dot3(q_of(0), split2(f_ref[3, :, span]))

    @pl.when(step == pl.num_programs(0) - 1)
    def _():
        for i in range(4):
            put_c[i].wait()


def last(flags, recv, q, shift, l, w1, w2, ath, atl, c, f):
    size = shift.shape[1]
    slots = w1.shape[1]
    cols = 256
    whole = pl.BlockSpec(memory_space=pltpu.VMEM)
    far = pl.BlockSpec(memory_space=pl.ANY)
    return pl.pallas_call(
        last_kernel,
        grid=(size // cols,),
        in_specs=[
            pl.BlockSpec(memory_space=pltpu.SMEM),
            whole, whole, whole, far, whole, far, whole, whole, far, whole,
        ],
        out_specs=(pl.BlockSpec((1, 3, size, cols), lambda n: (0, 0, 0, n)), far),
        out_shape=(
            jax.ShapeDtypeStruct((1, 3, size, size), F32),
            jax.ShapeDtypeStruct((1, 4, size, size), F32),
        ),
        scratch_shapes=[
            pltpu.VMEM(q.shape, F32),
            pltpu.VMEM((size, size), F32),
            pltpu.VMEM((4, size, size), F32),
            pltpu.VMEM((size, 3 * slots), BF16),
            pltpu.VMEM((size, 3 * slots), BF16),
            pltpu.SemaphoreType.DMA((2,)),
            pltpu.SemaphoreType.DMA((4,)),
            pltpu.SemaphoreType.DMA((4,)),
        ],
        compiler_params=pltpu.CompilerParams(vmem_limit_bytes=60 * 2**20),
        name="last",
    )(flags, recv, ath, atl, q, shift, l, w1, w2, c, f)


def exchange(payload):
    return lax.all_to_all(payload, AXES, split_axis=0, concat_axis=0, tiled=True)


def local(strips, index, shift, flags):
    count = lax.axis_size(AXES)
    own = lax.axis_index(AXES)
    strips = jnp.transpose(strips, (1, 0, 2))
    index = index.reshape(1, -1)
    first = bucket(first_kernel, "first", strips, index)
    recv = exchange(first)
    second = bucket(second_kernel, "second", strips, index, flags.reshape(1, -1))
    near = jnp.take(flags, (own + jnp.arange(-2, 6)) % count)
    wide = jnp.broadcast_to(near.astype(F32)[:, None], (8, 128))
    parts = chol(recv, shift, wide)
    q = exchange(second)
    return last(near, recv, q, shift, *parts)


def solution(mesh):
    in_specs = (P(AXES, None, None), P(AXES, None), P(AXES, None), P())
    out_specs = (P(AXES, None, None, None), P(AXES, None, None, None))
    return jax.shard_map(local, mesh=mesh, in_specs=in_specs, out_specs=out_specs, check_vma=False)
```

```python
import jax
import jax.numpy as jnp
from jax import lax
from jax.experimental import pallas as pl
from jax.experimental.pallas import tpu as pltpu
from jax.sharding import PartitionSpec as P

F32 = jnp.float32
BF16 = jnp.bfloat16
AXES = ("gx", "gy")


def split2(x):
    hi = x.astype(BF16)
    lo = (x - hi.astype(F32)).astype(BF16)
    return hi, lo


def dg(x, y, dims=((1,), (0,))):
    return lax.dot_general(x, y, (dims, ((), ())), preferred_element_type=F32)


def dot3(x, y, dims=((1,), (0,))):
    return dg(x[0], y[0], dims) + (dg(x[0], y[1], dims) + dg(x[1], y[0], dims))


def dot3_short(x, y):
    both = dg(jnp.concatenate(x, axis=1), jnp.concatenate([y[0], y[0]], axis=0))
    return both + dg(x[0], y[1])


def pieces_of(strips_ref):
    pieces = []
    for i in range(3):
        x = strips_ref[i]
        hi = x.astype(BF16)
        rest = x - hi.astype(F32)
        mid = rest.astype(BF16)
        low = (rest - mid.astype(F32)).astype(BF16)
        pieces.append((hi, mid, low))
    return pieces


def hits_of(row, slot):
    n = row.shape[1]
    r_id = lax.broadcasted_iota(jnp.int32, (n, n), 0)
    c_id = lax.broadcasted_iota(jnp.int32, (n, n), 1)
    wide = jnp.broadcast_to(row, (n, n))
    same = jnp.where((wide.T == wide) & (r_id < c_id), 1, 0)
    within = jnp.sum(same, axis=0, keepdims=True)
    return [(within == slot) & (((row + shift) & (n - 1)) == r_id) for shift in range(4)]


def as_mask(cond):
    return jnp.where(cond, 1.0, 0.0).astype(BF16)


def pick(select, piece):
    hi, mid, low = piece
    return dg(select, hi) + (dg(select, mid) + dg(select, low))


def first_kernel(strips_ref, row_ref, out_ref):
    width = strips_ref.shape[2]
    pieces = pieces_of(strips_ref)
    for slot in range(2):
        hit = hits_of(row_ref[...], slot)
        for i in range(3):
            out_ref[:, slot, i * width : (i + 1) * width] = pick(as_mask(hit[i]), pieces[i])


def second_kernel(strips_ref, row_ref, flag_ref, out_ref, near_ref, nearf_ref):
    width = strips_ref.shape[2]
    n = row_ref.shape[1]
    pieces = pieces_of(strips_ref)
    flags = flag_ref[...]
    r_id = lax.broadcasted_iota(jnp.int32, (n, n), 0)
    c_id = lax.broadcasted_iota(jnp.int32, (n, n), 1)

    def flag_before(step):
        chosen = c_id == ((r_id + (n - step)) & (n - 1))
        return jnp.sum(jnp.where(chosen, flags, 0), axis=1, keepdims=True) > 0

    own = lax.axis_index("gx") * lax.axis_size("gy") + lax.axis_index("gy")
    t_id = lax.broadcasted_iota(jnp.int32, (8, n), 0)
    l_id = lax.broadcasted_iota(jnp.int32, (8, n), 1)
    chosen = l_id == ((t_id + own + (n - 2)) & (n - 1))
    near = jnp.sum(jnp.where(chosen, flags, 0), axis=1, keepdims=True)
    near = jnp.broadcast_to(near, (8, n))
    near_ref[...] = near
    nearf_ref[...] = near.astype(F32)
    one_before = flag_before(1)
    two_before = flag_before(2)
    for slot in range(2):
        hit = hits_of(row_ref[...], slot)
        out_ref[:, slot, 0:width] = pick(as_mask(hit[1] & ~one_before), pieces[0]) + pick(
            as_mask(hit[3] & one_before), pieces[1]
        )
        out_ref[:, slot, width : 2 * width] = pick(as_mask(hit[2]), pieces[1])
        out_ref[:, slot, 2 * width : 3 * width] = pick(
            as_mask(hit[2] & ~two_before), pieces[0]
        ) + pick(as_mask(hit[3] & two_before), pieces[2])


def bucket(kernel, extra, *args):
    n, wide = args[0].shape[1], 3 * args[0].shape[2]
    return pl.pallas_call(
        kernel,
        out_shape=(jax.ShapeDtypeStruct((n, 2, wide), F32),) + extra,
        cost_estimate=pl.CostEstimate(
            flops=10 * n * n * wide, bytes_accessed=12 * n * wide, transcendentals=0
        ),
    )(*args)


def chol_block(a):
    n = a.shape[0]
    groups = n // 8
    sub = lax.broadcasted_iota(jnp.int32, (8, n), 0)
    lane = lax.broadcasted_iota(jnp.int32, (8, n), 1)
    left = [a[8 * v : 8 * v + 8, :] for v in range(groups)]
    right = [jnp.where(lane == sub + 8 * v, 1.0, 0.0).astype(F32) for v in range(groups)]

    def lanes_of(x, k):
        return [jnp.broadcast_to(x[:, 8 * k + i : 8 * k + i + 1], (8, n)) for i in range(8)]

    def sub_of(x, i):
        return jnp.broadcast_to(x[i : i + 1, :], (8, n))

    for k in range(groups):
        c = lanes_of(left[k], k)
        u, v_in = left[k], right[k]
        scale, row_u, row_v, row_c = [], [], [], []
        for i in range(8):
            inv = lax.rsqrt(sub_of(c[i], i))
            ru = sub_of(u, i) * inv
            rv = sub_of(v_in, i) * inv
            rc = [None] * 8
            m = jnp.where(sub > i, c[i] * inv, 0.0)
            for j in range(i + 1, 8):
                rc[j] = sub_of(c[j], i) * inv
                c[j] = c[j] - m * rc[j]
            u = jnp.where(sub == i, ru, u - m * ru)
            v_in = jnp.where(sub == i, rv, v_in - m * rv)
            scale.append(inv)
            row_u.append(ru)
            row_v.append(rv)
            row_c.append(rc)
        left[k], right[k] = u, v_in
        for g in range(k + 1, groups):
            c = lanes_of(left[g], k)
            x, y = left[g], right[g]
            for i in range(8):
                m = c[i] * scale[i]
                for j in range(i + 1, 8):
                    c[j] = c[j] - m * row_c[i][j]
                x = x - m * row_u[i]
                y = y - m * row_v[i]
            left[g], right[g] = x, y
    upper = jnp.concatenate(left, axis=0)
    r_id = lax.broadcasted_iota(jnp.int32, (n, n), 0)
    c_id = lax.broadcasted_iota(jnp.int32, (n, n), 1)
    return jnp.where(c_id >= r_id, upper, 0.0), jnp.concatenate(right, axis=0)


MESH = pl.DeviceIdType.MESH


def chol_kernel(
    recv_ref, shift_ref, flag_ref,
    lout_ref, w1out_ref, w2out_ref, athout_ref, atlout_ref, cout_ref, f_ref,
    l_ref, w1_ref, w2_ref, ath_ref, atl_ref, c_ref,
    m1w0_ref, m1w1_ref, m2w0_ref, p1w1_ref, p1w2_ref, p2w2_ref, gx_ref, gy_ref,
    m_ref, x_ref, w0_ref, ah_ref, al_ref, outx_ref, outy_ref, gram_ref,
    send_sem, recv_sem, small_send, small_recv, c_sem, o_sem,
):
    size = shift_ref.shape[1]
    slots = w0_ref.shape[1]
    half = slots // 2
    nb = 128
    count = size // nb
    rows_y = lax.axis_size("gy")
    total_dev = lax.axis_size("gx") * rows_y
    own = lax.axis_index("gx") * rows_y + lax.axis_index("gy")
    up = lax.rem(own + 1, total_dev)
    down = lax.rem(own + total_dev - 1, total_dev)
    up_id = (lax.div(up, rows_y), lax.rem(up, rows_y))
    down_id = (lax.div(down, rows_y), lax.rem(down, rows_y))

    barrier = pltpu.get_barrier_semaphore()
    for there in (up_id, down_id):
        pl.semaphore_signal(barrier, inc=1, device_id=there, device_id_type=MESH)

    def rows(k):
        return pl.ds(pl.multiple_of(k * nb, nb), nb)

    def copy(which, k):
        source, target, there = (
            (w0_ref, m1w0_ref, up_id),
            (w1_ref, m1w1_ref, up_id),
            (m1w0_ref, m2w0_ref, up_id),
            (w1_ref, p1w1_ref, down_id),
            (w2_ref, p1w2_ref, down_id),
            (p1w2_ref, p2w2_ref, down_id),
        )[which]
        return pltpu.make_async_remote_copy(
            src_ref=source.at[rows(k), :],
            dst_ref=target.at[rows(k), :],
            send_sem=send_sem.at[which, k],
            recv_sem=recv_sem.at[which, k],
            device_id=there,
            device_id_type=MESH,
        )

    def small(which):
        source, target = ((outx_ref, gx_ref), (outy_ref, gy_ref))[which]
        return pltpu.make_async_remote_copy(
            src_ref=source,
            dst_ref=target,
            send_sem=small_send.at[which],
            recv_sem=small_recv.at[which],
            device_id=up_id,
            device_id_type=MESH,
        )

    early = [
        pltpu.make_async_copy(source, target, o_sem.at[i])
        for i, (source, target) in enumerate(
            (
                (ath_ref, athout_ref), (atl_ref, atlout_ref),
                (l_ref, lout_ref), (w1_ref, w1out_ref), (w2_ref, w2out_ref),
            )
        )
    ]

    def relay(k):
        copy(0, k).wait_recv()
        copy(2, k).start()
        copy(4, k).wait_recv()
        copy(5, k).start()

    l_ref[...] = jnp.zeros_like(l_ref)
    f_ref[...] = jnp.zeros_like(f_ref)
    gram_ref[...] = jnp.zeros_like(gram_ref)
    for i in range(3):
        for s in range(2):
            x = recv_ref[:, s, i * size : (i + 1) * size]
            hi, lo = split2(x)
            ah_ref[i, s * half : (s + 1) * half, :] = hi
            al_ref[i, s * half : (s + 1) * half, :] = lo
            at = x.T
            begin = i * slots + s * half
            m_ref[:, size + begin : size + begin + half] = at
            hi, lo = split2(at)
            ath_ref[:, begin : begin + half] = hi
            atl_ref[:, begin : begin + half] = lo
    for blk in range(0, size, 256):
        total = None
        for i in range(3):
            a = (ah_ref[i, :, blk : blk + 256], al_ref[i, :, blk : blk + 256])
            here = slice(i * slots, (i + 1) * slots)
            t = (ath_ref[0 : blk + 256, here], atl_ref[0 : blk + 256, here])
            add = dot3(t, a)
            total = add if total is None else total + add
        r_id = lax.broadcasted_iota(jnp.int32, (blk + 256, 256), 0)
        c_id = lax.broadcasted_iota(jnp.int32, (blk + 256, 256), 1) + blk
        m_ref[0 : blk + 256, blk : blk + 256] = total + jnp.where(
            r_id == c_id, shift_ref[:, blk : blk + 256], 0.0
        )
    for i in range(2):
        early[i].start()
    pl.semaphore_wait(barrier, 2)

    w_refs = (w0_ref, w1_ref, w2_ref)

    def step(k, carry):
        at = pl.multiple_of(k * nb, nb)
        upper, inverse = chol_block(m_ref[pl.ds(at, nb), pl.ds(at, nb)])
        l_ref[pl.ds(at, nb), pl.ds(at, nb)] = upper.T
        inv = split2(inverse)
        for blk in range(size, 2 * size, 256):
            x_ref[:, blk : blk + 256] = dot3_short(
                inv, split2(m_ref[pl.ds(at, nb), blk : blk + 256])
            )
        for blk in range(0, size, 256):

            @pl.when(blk + 256 > at + nb)
            def _(blk=blk):
                x_ref[:, blk : blk + 256] = dot3_short(
                    inv, split2(m_ref[pl.ds(at, nb), blk : blk + 256])
                )
        for i in range(3):
            w_refs[i][pl.ds(at, nb), :] = x_ref[:, size + i * slots : size + (i + 1) * slots]

        def trail(r, inner):
            to = pl.multiple_of(r * nb, nb)
            low = x_ref[:, pl.ds(to, nb)].T
            l_ref[pl.ds(to, nb), pl.ds(at, nb)] = low
            low = split2(low)
            for blk in range(size, 2 * size, 256):
                m_ref[pl.ds(to, nb), blk : blk + 256] -= dot3_short(
                    low, split2(x_ref[:, blk : blk + 256])
                )
            for blk in range(0, size, 256):

                @pl.when(blk + 256 > to)
                def _(blk=blk):
                    m_ref[pl.ds(to, nb), blk : blk + 256] -= dot3_short(
                        low, split2(x_ref[:, blk : blk + 256])
                    )

            return inner

        lax.fori_loop(k + 1, count, trail, carry)
        wt = split2(x_ref[:, size + 2 * slots : size + 3 * slots].T)
        for j in range(2):
            gram_ref[j] += dot3_short(
                wt, split2(x_ref[:, size + j * slots : size + (j + 1) * slots])
            )
        for which in (0, 4, 1, 3):
            copy(which, k).start()

        @pl.when(k >= 2)
        def _():
            relay(k - 2)

        return carry

    lax.fori_loop(0, count, step, 0)

    flag = [flag_ref[i : i + 1, 0:1] for i in range(5)]
    outx_ref[...] = gram_ref[0] * flag[2]

    def a_of(i):
        return ah_ref[i], al_ref[i]

    def out_copy(which, k):
        return pltpu.make_async_copy(
            c_ref.at[which, wide(k), :], cout_ref.at[which, wide(k), :], c_sem.at[which, k]
        )

    def wide(k):
        return pl.ds(pl.multiple_of(k * 2 * nb, 2 * nb), 2 * nb)

    def near(k, carry):
        for part in range(2):
            copy(1, 2 * k + part).wait_recv()
            copy(3, 2 * k + part).wait_recv()

        @pl.when(k >= 1)
        def _():
            relay(k + 3)

        p1w1, p1w2 = p1w1_ref[wide(k), :], p1w2_ref[wide(k), :]
        c = dot3(split2(p1w1), a_of(0)) + dot3(split2(p1w2), a_of(1))
        c_ref[1, wide(k), :] = c
        c = split2(c * flag[3])
        f_ref[0] += dot3(split2(p1w1.T), c)
        f_ref[1] += dot3(split2(p1w2.T), c)

        @pl.when(k == 0)
        def _():
            small(0).start()

        m1w0, m1w1 = m1w0_ref[wide(k), :], m1w1_ref[wide(k), :]
        m1w0s = split2(m1w0)
        c = dot3(m1w0s, a_of(1)) + dot3(split2(m1w1), a_of(2))
        c_ref[2, wide(k), :] = c
        c = split2(c * flag[1])
        w1t = split2(m1w1.T)
        f_ref[1] += dot3(split2(m1w0.T), c)
        f_ref[2] += dot3(w1t, c)
        gram_ref[2] += dot3(w1t, m1w0s)
        out_copy(1, k).start()
        out_copy(2, k).start()
        return carry

    lax.fori_loop(0, count // 2, near, 0)
    for i in range(2, 5):
        early[i].start()
    outy_ref[...] = gram_ref[1] * flag[2] + gram_ref[2] * (1.0 - flag[2])

    def far(k, carry):
        for part in range(2):
            copy(2, 2 * k + part).wait_recv()
            copy(5, 2 * k + part).wait_recv()
        w = p2w2_ref[wide(k), :]
        c = dot3(split2(w), a_of(0))
        c_ref[0, wide(k), :] = c
        f_ref[0] += dot3(split2(w.T), split2(c * flag[4]))

        @pl.when(k == 0)
        def _():
            small(1).start()

        w = m2w0_ref[wide(k), :]
        c = dot3(split2(w), a_of(2))
        c_ref[3, wide(k), :] = c
        f_ref[2] += dot3(split2(w.T), split2(c * flag[0]))
        out_copy(0, k).start()
        out_copy(3, k).start()
        return carry

    lax.fori_loop(0, count // 2, far, 0)
    for which in range(2):
        small(which).wait_recv()
    f_ref[3] = dot3(split2(gx_ref[...]), a_of(1)) + dot3(split2(gy_ref[...]), a_of(2))
    for which in range(2):
        small(which).wait_send()
    for which in range(4):
        for k in range(count // 2):
            out_copy(which, k).wait()
    for i in range(5):
        early[i].wait()

    def drain(k, carry):
        for which in range(6):
            copy(which, k).wait_send()
        return carry

    lax.fori_loop(0, count, drain, 0)


def chol(recv, shift, flags):
    size = shift.shape[1]
    slots = 2 * recv.shape[0]
    w = jax.ShapeDtypeStruct((size, slots), F32)
    low = jax.ShapeDtypeStruct((size, 3 * slots), BF16)
    count = size // 128
    whole = pl.BlockSpec(memory_space=pltpu.VMEM)
    return pl.pallas_call(
        chol_kernel,
        out_shape=(
            jax.ShapeDtypeStruct((size, size), F32), w, w, low, low,
            jax.ShapeDtypeStruct((4, size, size), F32),
            jax.ShapeDtypeStruct((4, slots, size), F32),
        ),
        out_specs=(pl.BlockSpec(memory_space=pl.ANY),) * 6 + (whole,),
        scratch_shapes=[
            pltpu.VMEM((size, size), F32),
            pltpu.VMEM((size, slots), F32),
            pltpu.VMEM((size, slots), F32),
            pltpu.VMEM((size, 3 * slots), BF16),
            pltpu.VMEM((size, 3 * slots), BF16),
            pltpu.VMEM((4, size, size), F32),
        ]
        + [pltpu.VMEM((size, slots), F32)] * 6
        + [pltpu.VMEM((slots, slots), F32)] * 2
        + [
            pltpu.VMEM((size, size + 3 * slots), F32),
            pltpu.VMEM((128, size + 3 * slots), F32),
            pltpu.VMEM((size, slots), F32),
            pltpu.VMEM((3, slots, size), BF16),
            pltpu.VMEM((3, slots, size), BF16),
            pltpu.VMEM((slots, slots), F32),
            pltpu.VMEM((slots, slots), F32),
            pltpu.VMEM((3, slots, slots), F32),
            pltpu.SemaphoreType.DMA((6, count)),
            pltpu.SemaphoreType.DMA((6, count)),
            pltpu.SemaphoreType.DMA((2,)),
            pltpu.SemaphoreType.DMA((2,)),
            pltpu.SemaphoreType.DMA((4, count // 2)),
            pltpu.SemaphoreType.DMA((5,)),
        ],
        compiler_params=pltpu.CompilerParams(
            vmem_limit_bytes=60 * 2**20, collective_id=0, has_side_effects=True
        ),
        cost_estimate=pl.CostEstimate(
            flops=30 * size * size * size, bytes_accessed=30 * size * size, transcendentals=0
        ),
        name="chol",
    )(recv, shift, flags)


def last_kernel(
    flag_ref, recv_ref, ath_ref, atl_ref, qin_ref, shift_ref, lin_ref, w1in_ref, w2in_ref, cin_ref, f_ref,
    schur_ref, coup_ref, q_ref, l_ref, w1_ref, w2_ref, c_ref, qh_ref, ql_ref, sem, in_sem, out_sem,
):
    step = pl.program_id(0)
    size = shift_ref.shape[1]
    slots = w1_ref.shape[1]
    half = slots // 2
    cols = schur_ref.shape[3]
    fm2, fm1, own = [flag_ref[i, 0] > 0 for i in range(3)]
    get_q = pltpu.make_async_copy(qin_ref, q_ref, sem.at[0])
    get_own = [
        pltpu.make_async_copy(lin_ref, l_ref, sem.at[1]),
        pltpu.make_async_copy(w1in_ref, w1_ref, sem.at[2]),
        pltpu.make_async_copy(w2in_ref, w2_ref, sem.at[3]),
    ]
    get_c = [pltpu.make_async_copy(cin_ref.at[i], c_ref.at[i], in_sem.at[i]) for i in range(4)]
    put_c = [pltpu.make_async_copy(c_ref.at[i], coup_ref.at[0, i], out_sem.at[i]) for i in range(4)]

    @pl.when(step == 0)
    def _():
        get_q.start()

        @pl.when(own)
        def _():
            for one in get_own:
                one.start()

        for i in (2, 3, 0, 1):
            get_c[i].start()

    base = pl.multiple_of(step * cols, cols)
    span = pl.ds(base, cols)

    def at_of(i):
        return ath_ref[:, i * slots : (i + 1) * slots], atl_ref[:, i * slots : (i + 1) * slots]

    def q_of(i):
        return qh_ref[:, i * slots : (i + 1) * slots], ql_ref[:, i * slots : (i + 1) * slots]

    def y_of(i):
        lanes = pl.ds(pl.multiple_of(i * size + base, cols), cols)
        a = jnp.concatenate([recv_ref[:, 0, lanes], recv_ref[:, 1, lanes]], axis=0)
        return split2(a - f_ref[i, :, span])

    @pl.when(jnp.logical_not(own))
    def _():
        r_id = lax.broadcasted_iota(jnp.int32, (size, cols), 0)
        c_id = lax.broadcasted_iota(jnp.int32, (size, cols), 1) + base
        diag = jnp.where(r_id == c_id, shift_ref[:, span], 0.0)
        schur_ref[0, 2] = (
            dot3(at_of(0), y_of(0)) + dot3(at_of(1), y_of(1)) + dot3(at_of(2), y_of(2))
        ) + diag

    @pl.when(step == 0)
    def _():
        get_q.wait()
        for i in range(3):
            for s in range(2):
                begin = i * slots + s * half
                hi, lo = split2(q_ref[:, s, i * size : (i + 1) * size].T)
                qh_ref[:, begin : begin + half] = hi
                ql_ref[:, begin : begin + half] = lo

        @pl.when(own)
        def _():
            for one in get_own:
                one.wait()

        for i in (2, 3, 0, 1):
            get_c[i].wait()
            put_c[i].start()

    @pl.when(own)
    def _():
        w1 = split2(w1_ref[span, :])
        w2 = split2(w2_ref[span, :])
        over = ((1,), (1,))
        schur_ref[0, 0] = dot3(q_of(2), w2, over)
        schur_ref[0, 1] = dot3(q_of(0), w1, over) + dot3(q_of(1), w2, over)
        schur_ref[0, 2] = l_ref[:, span]

    @pl.when(jnp.logical_not(own))
    def _():
        @pl.when(fm1)
        def _():
            schur_ref[0, 1] = c_ref[2, :, span]

        @pl.when(jnp.logical_not(fm1))
        def _():
            schur_ref[0, 1] = dot3(q_of(0), y_of(1)) + dot3(q_of(1), y_of(2))

            @pl.when(fm2)
            def _():
                schur_ref[0, 1] -= dot3(q_of(2), split2(f_ref[3, :, span]))

        @pl.when(fm2)
        def _():
            schur_ref[0, 0] = c_ref[3, :, span]

        @pl.when(jnp.logical_not(fm2))
        def _():
            schur_ref[0, 0] = dot3(q_of(2), y_of(2))

            @pl.when(fm1)
            def _():
                schur_ref[0, 0] -= dot3(q_of(0), split2(f_ref[3, :, span]))

    @pl.when(step == pl.num_programs(0) - 1)
    def _():
        for i in range(4):
            put_c[i].wait()


def last(flags, recv, q, shift, l, w1, w2, ath, atl, c, f):
    size = shift.shape[1]
    slots = w1.shape[1]
    cols = 256
    whole = pl.BlockSpec(memory_space=pltpu.VMEM)
    far = pl.BlockSpec(memory_space=pl.ANY)
    return pl.pallas_call(
        last_kernel,
        grid=(size // cols,),
        in_specs=[
            pl.BlockSpec(memory_space=pltpu.SMEM),
            whole, whole, whole, far, whole, far, far, far, far, whole,
        ],
        out_specs=(pl.BlockSpec((1, 3, size, cols), lambda n: (0, 0, 0, n)), far),
        out_shape=(
            jax.ShapeDtypeStruct((1, 3, size, size), F32),
            jax.ShapeDtypeStruct((1, 4, size, size), F32),
        ),
        scratch_shapes=[
            pltpu.VMEM(q.shape, F32),
            pltpu.VMEM((size, size), F32),
            pltpu.VMEM((size, slots), F32),
            pltpu.VMEM((size, slots), F32),
            pltpu.VMEM((4, size, size), F32),
            pltpu.VMEM((size, 3 * slots), BF16),
            pltpu.VMEM((size, 3 * slots), BF16),
            pltpu.SemaphoreType.DMA((4,)),
            pltpu.SemaphoreType.DMA((4,)),
            pltpu.SemaphoreType.DMA((4,)),
        ],
        compiler_params=pltpu.CompilerParams(vmem_limit_bytes=60 * 2**20),
        name="last",
    )(flags, recv, ath, atl, q, shift, l, w1, w2, c, f)


def exchange(payload):
    return lax.all_to_all(payload, AXES, split_axis=0, concat_axis=0, tiled=True)


def local(strips, index, shift, flags):
    strips = jnp.transpose(strips, (1, 0, 2))
    index = index.reshape(1, -1)
    (first,) = bucket(first_kernel, (), strips, index)
    table = (8, flags.shape[0])
    extra = (jax.ShapeDtypeStruct(table, jnp.int32), jax.ShapeDtypeStruct(table, F32))
    second, near, wide = bucket(second_kernel, extra, strips, index, flags.reshape(1, -1))
    recv = exchange(first)
    q = exchange(second)
    parts = chol(recv, shift, wide)
    return last(near, recv, q, shift, *parts)


def solution(mesh):
    in_specs = (P(AXES, None, None), P(AXES, None), P(AXES, None), P())
    out_specs = (P(AXES, None, None, None), P(AXES, None, None, None))
    return jax.shard_map(local, mesh=mesh, in_specs=in_specs, out_specs=out_specs, check_vma=False)
```

```python
import jax
import jax.numpy as jnp
from jax import lax
from jax.experimental import pallas as pl
from jax.experimental.pallas import tpu as pltpu
from jax.sharding import PartitionSpec as P

F32 = jnp.float32
BF16 = jnp.bfloat16
AXES = ("gx", "gy")


def split2(x):
    hi = x.astype(BF16)
    lo = (x - hi.astype(F32)).astype(BF16)
    return hi, lo


def dg(x, y, dims=((1,), (0,))):
    return lax.dot_general(x, y, (dims, ((), ())), preferred_element_type=F32)


def dot3(x, y, dims=((1,), (0,))):
    return dg(x[0], y[0], dims) + (dg(x[0], y[1], dims) + dg(x[1], y[0], dims))


def dot3_short(x, y):
    both = dg(jnp.concatenate(x, axis=1), jnp.concatenate([y[0], y[0]], axis=0))
    return both + dg(x[0], y[1])


def pieces_of(strips_ref):
    pieces = []
    for i in range(3):
        x = strips_ref[i]
        hi = x.astype(BF16)
        rest = x - hi.astype(F32)
        mid = rest.astype(BF16)
        low = (rest - mid.astype(F32)).astype(BF16)
        pieces.append((hi, mid, low))
    return pieces


def hits_of(row, slot):
    n = row.shape[1]
    r_id = lax.broadcasted_iota(jnp.int32, (n, n), 0)
    c_id = lax.broadcasted_iota(jnp.int32, (n, n), 1)
    wide = jnp.broadcast_to(row, (n, n))
    same = jnp.where((wide.T == wide) & (r_id < c_id), 1, 0)
    within = jnp.sum(same, axis=0, keepdims=True)
    return [(within == slot) & (((row + shift) & (n - 1)) == r_id) for shift in range(4)]


def as_mask(cond):
    return jnp.where(cond, 1.0, 0.0).astype(BF16)


def pick(select, piece):
    hi, mid, low = piece
    return dg(select, hi) + (dg(select, mid) + dg(select, low))


def first_kernel(strips_ref, row_ref, out_ref):
    width = strips_ref.shape[2]
    pieces = pieces_of(strips_ref)
    n = row_ref.shape[1]
    hits = [hits_of(row_ref[...], slot) for slot in range(2)]
    for i in range(3):
        both = jnp.concatenate([as_mask(hit[i]) for hit in hits], axis=0)
        rows = pick(both, pieces[i])
        for slot in range(2):
            out_ref[:, slot, i * width : (i + 1) * width] = rows[slot * n : (slot + 1) * n]


def second_kernel(strips_ref, row_ref, flag_ref, out_ref, near_ref, nearf_ref):
    width = strips_ref.shape[2]
    n = row_ref.shape[1]
    pieces = pieces_of(strips_ref)
    flags = flag_ref[...]
    r_id = lax.broadcasted_iota(jnp.int32, (n, n), 0)
    c_id = lax.broadcasted_iota(jnp.int32, (n, n), 1)

    def flag_before(step):
        chosen = c_id == ((r_id + (n - step)) & (n - 1))
        return jnp.sum(jnp.where(chosen, flags, 0), axis=1, keepdims=True) > 0

    own = lax.axis_index("gx") * lax.axis_size("gy") + lax.axis_index("gy")
    t_id = lax.broadcasted_iota(jnp.int32, (8, n), 0)
    l_id = lax.broadcasted_iota(jnp.int32, (8, n), 1)
    chosen = l_id == ((t_id + own + (n - 2)) & (n - 1))
    near = jnp.sum(jnp.where(chosen, flags, 0), axis=1, keepdims=True)
    near = jnp.broadcast_to(near, (8, n))
    near_ref[...] = near
    nearf_ref[...] = near.astype(F32)
    one_before = flag_before(1)
    two_before = flag_before(2)
    for slot in range(2):
        hit = hits_of(row_ref[...], slot)
        out_ref[:, slot, 0:width] = pick(as_mask(hit[1] & ~one_before), pieces[0]) + pick(
            as_mask(hit[3] & one_before), pieces[1]
        )
        out_ref[:, slot, width : 2 * width] = pick(as_mask(hit[2]), pieces[1])
        out_ref[:, slot, 2 * width : 3 * width] = pick(
            as_mask(hit[2] & ~two_before), pieces[0]
        ) + pick(as_mask(hit[3] & two_before), pieces[2])


def bucket(kernel, extra, *args):
    n, wide = args[0].shape[1], 3 * args[0].shape[2]
    return pl.pallas_call(
        kernel,
        out_shape=(jax.ShapeDtypeStruct((n, 2, wide), F32),) + extra,
        cost_estimate=pl.CostEstimate(
            flops=10 * n * n * wide, bytes_accessed=12 * n * wide, transcendentals=0
        ),
        compiler_params=pltpu.CompilerParams(vmem_limit_bytes=62 * 2**20),
    )(*args)


def chol_block(a):
    n = a.shape[0]
    groups = n // 8
    sub = lax.broadcasted_iota(jnp.int32, (8, n), 0)
    lane = lax.broadcasted_iota(jnp.int32, (8, n), 1)
    left = [a[8 * v : 8 * v + 8, :] for v in range(groups)]
    right = [jnp.where(lane == sub + 8 * v, 1.0, 0.0).astype(F32) for v in range(groups)]

    def lanes_of(x, k):
        return [jnp.broadcast_to(x[:, 8 * k + i : 8 * k + i + 1], (8, n)) for i in range(8)]

    def sub_of(x, i):
        return jnp.broadcast_to(x[i : i + 1, :], (8, n))

    for k in range(groups):
        c = lanes_of(left[k], k)
        u, v_in = left[k], right[k]
        scale, row_u, row_v, row_c = [], [], [], []
        for i in range(8):
            inv = lax.rsqrt(sub_of(c[i], i))
            ru = sub_of(u, i) * inv
            rv = sub_of(v_in, i) * inv
            rc = [None] * 8
            m = jnp.where(sub > i, c[i] * inv, 0.0)
            for j in range(i + 1, 8):
                rc[j] = sub_of(c[j], i) * inv
                c[j] = c[j] - m * rc[j]
            u = jnp.where(sub == i, ru, u - m * ru)
            v_in = jnp.where(sub == i, rv, v_in - m * rv)
            scale.append(inv)
            row_u.append(ru)
            row_v.append(rv)
            row_c.append(rc)
        left[k], right[k] = u, v_in
        for g in range(k + 1, groups):
            c = lanes_of(left[g], k)
            x, y = left[g], right[g]
            for i in range(8):
                m = c[i] * scale[i]
                for j in range(i + 1, 8):
                    c[j] = c[j] - m * row_c[i][j]
                x = x - m * row_u[i]
                y = y - m * row_v[i]
            left[g], right[g] = x, y
    upper = jnp.concatenate(left, axis=0)
    r_id = lax.broadcasted_iota(jnp.int32, (n, n), 0)
    c_id = lax.broadcasted_iota(jnp.int32, (n, n), 1)
    return jnp.where(c_id >= r_id, upper, 0.0), jnp.concatenate(right, axis=0)


MESH = pl.DeviceIdType.MESH


def chol_kernel(
    recv_ref, shift_ref, flag_ref,
    lout_ref, w1out_ref, w2out_ref, athout_ref, atlout_ref, cout_ref, f_ref,
    l_ref, w1_ref, w2_ref, ath_ref, atl_ref, c_ref,
    m1w0_ref, m1w1_ref, m2w0_ref, p1w1_ref, p1w2_ref, p2w2_ref, gx_ref, gy_ref,
    m_ref, x_ref, w0_ref, ah_ref, al_ref, outx_ref, outy_ref, gram_ref,
    send_sem, recv_sem, small_send, small_recv, c_sem, o_sem,
):
    size = shift_ref.shape[1]
    slots = w0_ref.shape[1]
    half = slots // 2
    nb = 128
    count = size // nb
    rows_y = lax.axis_size("gy")
    total_dev = lax.axis_size("gx") * rows_y
    own = lax.axis_index("gx") * rows_y + lax.axis_index("gy")
    up = lax.rem(own + 1, total_dev)
    down = lax.rem(own + total_dev - 1, total_dev)
    up_id = (lax.div(up, rows_y), lax.rem(up, rows_y))
    down_id = (lax.div(down, rows_y), lax.rem(down, rows_y))

    barrier = pltpu.get_barrier_semaphore()
    for there in (up_id, down_id):
        pl.semaphore_signal(barrier, inc=1, device_id=there, device_id_type=MESH)

    def rows(k):
        return pl.ds(pl.multiple_of(k * nb, nb), nb)

    def copy(which, k):
        source, target, there = (
            (w0_ref, m1w0_ref, up_id),
            (w1_ref, m1w1_ref, up_id),
            (m1w0_ref, m2w0_ref, up_id),
            (w1_ref, p1w1_ref, down_id),
            (w2_ref, p1w2_ref, down_id),
            (p1w2_ref, p2w2_ref, down_id),
        )[which]
        return pltpu.make_async_remote_copy(
            src_ref=source.at[rows(k), :],
            dst_ref=target.at[rows(k), :],
            send_sem=send_sem.at[which, k],
            recv_sem=recv_sem.at[which, k],
            device_id=there,
            device_id_type=MESH,
        )

    def small(which):
        source, target = ((outx_ref, gx_ref), (outy_ref, gy_ref))[which]
        return pltpu.make_async_remote_copy(
            src_ref=source,
            dst_ref=target,
            send_sem=small_send.at[which],
            recv_sem=small_recv.at[which],
            device_id=up_id,
            device_id_type=MESH,
        )

    early = [
        pltpu.make_async_copy(source, target, o_sem.at[i])
        for i, (source, target) in enumerate(
            (
                (ath_ref, athout_ref), (atl_ref, atlout_ref),
                (l_ref, lout_ref), (w1_ref, w1out_ref), (w2_ref, w2out_ref),
            )
        )
    ]

    def relay(k):
        copy(0, k).wait_recv()
        copy(2, k).start()
        copy(4, k).wait_recv()
        copy(5, k).start()

    l_ref[...] = jnp.zeros_like(l_ref)
    f_ref[...] = jnp.zeros_like(f_ref)
    gram_ref[...] = jnp.zeros_like(gram_ref)
    for i in range(3):
        for s in range(2):
            x = recv_ref[:, s, i * size : (i + 1) * size]
            hi, lo = split2(x)
            ah_ref[i, s * half : (s + 1) * half, :] = hi
            al_ref[i, s * half : (s + 1) * half, :] = lo
            at = x.T
            begin = i * slots + s * half
            m_ref[:, size + begin : size + begin + half] = at
            hi, lo = split2(at)
            ath_ref[:, begin : begin + half] = hi
            atl_ref[:, begin : begin + half] = lo
    for blk in range(0, size, 256):
        total = None
        for i in range(3):
            a = (ah_ref[i, :, blk : blk + 256], al_ref[i, :, blk : blk + 256])
            here = slice(i * slots, (i + 1) * slots)
            t = (ath_ref[0 : blk + 256, here], atl_ref[0 : blk + 256, here])
            add = dot3(t, a)
            total = add if total is None else total + add
        r_id = lax.broadcasted_iota(jnp.int32, (blk + 256, 256), 0)
        c_id = lax.broadcasted_iota(jnp.int32, (blk + 256, 256), 1) + blk
        m_ref[0 : blk + 256, blk : blk + 256] = total + jnp.where(
            r_id == c_id, shift_ref[:, blk : blk + 256], 0.0
        )
    for i in range(2):
        early[i].start()
    pl.semaphore_wait(barrier, 2)

    w_refs = (w0_ref, w1_ref, w2_ref)

    def step(k, carry):
        at = pl.multiple_of(k * nb, nb)
        upper, inverse = chol_block(m_ref[pl.ds(at, nb), pl.ds(at, nb)])
        l_ref[pl.ds(at, nb), pl.ds(at, nb)] = upper.T
        inv = split2(inverse)
        for blk in range(size, 2 * size, 256):
            x_ref[:, blk : blk + 256] = dot3_short(
                inv, split2(m_ref[pl.ds(at, nb), blk : blk + 256])
            )
        for blk in range(0, size, 256):

            @pl.when(blk + 256 > at + nb)
            def _(blk=blk):
                x_ref[:, blk : blk + 256] = dot3_short(
                    inv, split2(m_ref[pl.ds(at, nb), blk : blk + 256])
                )
        for i in range(3):
            w_refs[i][pl.ds(at, nb), :] = x_ref[:, size + i * slots : size + (i + 1) * slots]

        def trail(r, inner):
            to = pl.multiple_of(r * nb, nb)
            low = x_ref[:, pl.ds(to, nb)].T
            l_ref[pl.ds(to, nb), pl.ds(at, nb)] = low
            low = split2(low)
            for blk in range(size, 2 * size, 256):
                m_ref[pl.ds(to, nb), blk : blk + 256] -= dot3_short(
                    low, split2(x_ref[:, blk : blk + 256])
                )
            for blk in range(0, size, 256):

                @pl.when(blk + 256 > to)
                def _(blk=blk):
                    m_ref[pl.ds(to, nb), blk : blk + 256] -= dot3_short(
                        low, split2(x_ref[:, blk : blk + 256])
                    )

            return inner

        lax.fori_loop(k + 1, count, trail, carry)
        wt = split2(x_ref[:, size + 2 * slots : size + 3 * slots].T)
        for j in range(2):
            gram_ref[j] += dot3_short(
                wt, split2(x_ref[:, size + j * slots : size + (j + 1) * slots])
            )
        for which in (0, 4, 1, 3):
            copy(which, k).start()

        @pl.when(k >= 2)
        def _():
            relay(k - 2)

        return carry

    lax.fori_loop(0, count, step, 0)

    flag = [flag_ref[i : i + 1, 0:1] for i in range(5)]
    outx_ref[...] = gram_ref[0] * flag[2]

    def a_of(i):
        return ah_ref[i], al_ref[i]

    def out_copy(which, k):
        return pltpu.make_async_copy(
            c_ref.at[which, wide(k), :], cout_ref.at[which, wide(k), :], c_sem.at[which, k]
        )

    def wide(k):
        return pl.ds(pl.multiple_of(k * 2 * nb, 2 * nb), 2 * nb)

    def near(k, carry):
        for part in range(2):
            copy(1, 2 * k + part).wait_recv()
            copy(3, 2 * k + part).wait_recv()

        @pl.when(k >= 1)
        def _():
            relay(k + 3)

        p1w1, p1w2 = p1w1_ref[wide(k), :], p1w2_ref[wide(k), :]
        c = dot3(split2(p1w1), a_of(0)) + dot3(split2(p1w2), a_of(1))
        c_ref[1, wide(k), :] = c
        c = split2(c * flag[3])
        f_ref[0] += dot3(split2(p1w1.T), c)
        f_ref[1] += dot3(split2(p1w2.T), c)

        @pl.when(k == 0)
        def _():
            small(0).start()

        m1w0, m1w1 = m1w0_ref[wide(k), :], m1w1_ref[wide(k), :]
        m1w0s = split2(m1w0)
        c = dot3(m1w0s, a_of(1)) + dot3(split2(m1w1), a_of(2))
        c_ref[2, wide(k), :] = c
        c = split2(c * flag[1])
        w1t = split2(m1w1.T)
        f_ref[1] += dot3(split2(m1w0.T), c)
        f_ref[2] += dot3(w1t, c)
        gram_ref[2] += dot3(w1t, m1w0s)
        out_copy(1, k).start()
        out_copy(2, k).start()
        return carry

    lax.fori_loop(0, count // 2, near, 0)
    for i in range(2, 5):
        early[i].start()
    outy_ref[...] = gram_ref[1] * flag[2] + gram_ref[2] * (1.0 - flag[2])

    def far(k, carry):
        for part in range(2):
            copy(2, 2 * k + part).wait_recv()
            copy(5, 2 * k + part).wait_recv()
        w = p2w2_ref[wide(k), :]
        c = dot3(split2(w), a_of(0))
        c_ref[0, wide(k), :] = c
        f_ref[0] += dot3(split2(w.T), split2(c * flag[4]))

        @pl.when(k == 0)
        def _():
            small(1).start()

        w = m2w0_ref[wide(k), :]
        c = dot3(split2(w), a_of(2))
        c_ref[3, wide(k), :] = c
        f_ref[2] += dot3(split2(w.T), split2(c * flag[0]))
        out_copy(0, k).start()
        out_copy(3, k).start()
        return carry

    lax.fori_loop(0, count // 2, far, 0)
    for which in range(2):
        small(which).wait_recv()
    f_ref[3] = dot3(split2(gx_ref[...]), a_of(1)) + dot3(split2(gy_ref[...]), a_of(2))
    for which in range(2):
        small(which).wait_send()
    for which in range(4):
        for k in range(count // 2):
            out_copy(which, k).wait()
    for i in range(5):
        early[i].wait()

    def drain(k, carry):
        for which in range(6):
            copy(which, k).wait_send()
        return carry

    lax.fori_loop(0, count, drain, 0)


def chol(recv, shift, flags):
    size = shift.shape[1]
    slots = 2 * recv.shape[0]
    w = jax.ShapeDtypeStruct((size, slots), F32)
    low = jax.ShapeDtypeStruct((size, 3 * slots), BF16)
    count = size // 128
    whole = pl.BlockSpec(memory_space=pltpu.VMEM)
    return pl.pallas_call(
        chol_kernel,
        out_shape=(
            jax.ShapeDtypeStruct((size, size), F32), w, w, low, low,
            jax.ShapeDtypeStruct((4, size, size), F32),
            jax.ShapeDtypeStruct((4, slots, size), F32),
        ),
        out_specs=(pl.BlockSpec(memory_space=pl.ANY),) * 6 + (whole,),
        scratch_shapes=[
            pltpu.VMEM((size, size), F32),
            pltpu.VMEM((size, slots), F32),
            pltpu.VMEM((size, slots), F32),
            pltpu.VMEM((size, 3 * slots), BF16),
            pltpu.VMEM((size, 3 * slots), BF16),
            pltpu.VMEM((4, size, size), F32),
        ]
        + [pltpu.VMEM((size, slots), F32)] * 6
        + [pltpu.VMEM((slots, slots), F32)] * 2
        + [
            pltpu.VMEM((size, size + 3 * slots), F32),
            pltpu.VMEM((128, size + 3 * slots), F32),
            pltpu.VMEM((size, slots), F32),
            pltpu.VMEM((3, slots, size), BF16),
            pltpu.VMEM((3, slots, size), BF16),
            pltpu.VMEM((slots, slots), F32),
            pltpu.VMEM((slots, slots), F32),
            pltpu.VMEM((3, slots, slots), F32),
            pltpu.SemaphoreType.DMA((6, count)),
            pltpu.SemaphoreType.DMA((6, count)),
            pltpu.SemaphoreType.DMA((2,)),
            pltpu.SemaphoreType.DMA((2,)),
            pltpu.SemaphoreType.DMA((4, count // 2)),
            pltpu.SemaphoreType.DMA((5,)),
        ],
        compiler_params=pltpu.CompilerParams(
            vmem_limit_bytes=62 * 2**20, collective_id=0, has_side_effects=True
        ),
        cost_estimate=pl.CostEstimate(
            flops=30 * size * size * size, bytes_accessed=30 * size * size, transcendentals=0
        ),
        name="chol",
    )(recv, shift, flags)


def last_kernel(
    flag_ref, recv_ref, ath_ref, atl_ref, qin_ref, shift_ref, lin_ref, w1in_ref, w2in_ref, cin_ref, f_ref,
    schur_ref, coup_ref, q_ref, l_ref, w1_ref, w2_ref, c_ref, qh_ref, ql_ref, sem, in_sem, out_sem,
):
    step = pl.program_id(0)
    size = shift_ref.shape[1]
    slots = w1_ref.shape[1]
    half = slots // 2
    cols = schur_ref.shape[3]
    fm2, fm1, own = [flag_ref[i, 0] > 0 for i in range(3)]
    get_q = pltpu.make_async_copy(qin_ref, q_ref, sem.at[0])
    get_own = [
        pltpu.make_async_copy(lin_ref, l_ref, sem.at[1]),
        pltpu.make_async_copy(w1in_ref, w1_ref, sem.at[2]),
        pltpu.make_async_copy(w2in_ref, w2_ref, sem.at[3]),
    ]
    get_c = [pltpu.make_async_copy(cin_ref.at[i], c_ref.at[i], in_sem.at[i]) for i in range(4)]
    put_c = [pltpu.make_async_copy(c_ref.at[i], coup_ref.at[0, i], out_sem.at[i]) for i in range(4)]

    @pl.when(step == 0)
    def _():
        get_q.start()

        @pl.when(own)
        def _():
            for one in get_own:
                one.start()

        for i in (2, 3, 0, 1):
            get_c[i].start()

    base = pl.multiple_of(step * cols, cols)
    span = pl.ds(base, cols)

    def at_of(i):
        return ath_ref[:, i * slots : (i + 1) * slots], atl_ref[:, i * slots : (i + 1) * slots]

    def q_of(i):
        return qh_ref[:, i * slots : (i + 1) * slots], ql_ref[:, i * slots : (i + 1) * slots]

    def y_of(i):
        lanes = pl.ds(pl.multiple_of(i * size + base, cols), cols)
        a = jnp.concatenate([recv_ref[:, 0, lanes], recv_ref[:, 1, lanes]], axis=0)
        return split2(a - f_ref[i, :, span])

    @pl.when(jnp.logical_not(own))
    def _():
        r_id = lax.broadcasted_iota(jnp.int32, (size, cols), 0)
        c_id = lax.broadcasted_iota(jnp.int32, (size, cols), 1) + base
        diag = jnp.where(r_id == c_id, shift_ref[:, span], 0.0)
        schur_ref[0, 2] = (
            dot3(at_of(0), y_of(0)) + dot3(at_of(1), y_of(1)) + dot3(at_of(2), y_of(2))
        ) + diag

    @pl.when(step == 0)
    def _():
        get_q.wait()
        for i in range(3):
            for s in range(2):
                begin = i * slots + s * half
                hi, lo = split2(q_ref[:, s, i * size : (i + 1) * size].T)
                qh_ref[:, begin : begin + half] = hi
                ql_ref[:, begin : begin + half] = lo

        @pl.when(own)
        def _():
            for one in get_own:
                one.wait()

        for i in (2, 3, 0, 1):
            get_c[i].wait()
            put_c[i].start()

    @pl.when(own)
    def _():
        w1 = split2(w1_ref[span, :])
        w2 = split2(w2_ref[span, :])
        over = ((1,), (1,))
        schur_ref[0, 0] = dot3(q_of(2), w2, over)
        schur_ref[0, 1] = dot3(q_of(0), w1, over) + dot3(q_of(1), w2, over)
        schur_ref[0, 2] = l_ref[:, span]

    @pl.when(jnp.logical_not(own))
    def _():
        @pl.when(fm1)
        def _():
            schur_ref[0, 1] = c_ref[2, :, span]

        @pl.when(jnp.logical_not(fm1))
        def _():
            schur_ref[0, 1] = dot3(q_of(0), y_of(1)) + dot3(q_of(1), y_of(2))

            @pl.when(fm2)
            def _():
                schur_ref[0, 1] -= dot3(q_of(2), split2(f_ref[3, :, span]))

        @pl.when(fm2)
        def _():
            schur_ref[0, 0] = c_ref[3, :, span]

        @pl.when(jnp.logical_not(fm2))
        def _():
            schur_ref[0, 0] = dot3(q_of(2), y_of(2))

            @pl.when(fm1)
            def _():
                schur_ref[0, 0] -= dot3(q_of(0), split2(f_ref[3, :, span]))

    @pl.when(step == pl.num_programs(0) - 1)
    def _():
        for i in range(4):
            put_c[i].wait()


def last(flags, recv, q, shift, l, w1, w2, ath, atl, c, f):
    size = shift.shape[1]
    slots = w1.shape[1]
    cols = 256
    whole = pl.BlockSpec(memory_space=pltpu.VMEM)
    far = pl.BlockSpec(memory_space=pl.ANY)
    return pl.pallas_call(
        last_kernel,
        grid=(size // cols,),
        in_specs=[
            pl.BlockSpec(memory_space=pltpu.SMEM),
            whole, whole, whole, far, whole, far, far, far, far, whole,
        ],
        out_specs=(pl.BlockSpec((1, 3, size, cols), lambda n: (0, 0, 0, n)), far),
        out_shape=(
            jax.ShapeDtypeStruct((1, 3, size, size), F32),
            jax.ShapeDtypeStruct((1, 4, size, size), F32),
        ),
        scratch_shapes=[
            pltpu.VMEM(q.shape, F32),
            pltpu.VMEM((size, size), F32),
            pltpu.VMEM((size, slots), F32),
            pltpu.VMEM((size, slots), F32),
            pltpu.VMEM((4, size, size), F32),
            pltpu.VMEM((size, 3 * slots), BF16),
            pltpu.VMEM((size, 3 * slots), BF16),
            pltpu.SemaphoreType.DMA((4,)),
            pltpu.SemaphoreType.DMA((4,)),
            pltpu.SemaphoreType.DMA((4,)),
        ],
        compiler_params=pltpu.CompilerParams(vmem_limit_bytes=62 * 2**20),
        name="last",
    )(flags, recv, ath, atl, q, shift, l, w1, w2, c, f)


def exchange(payload):
    return lax.all_to_all(payload, AXES, split_axis=0, concat_axis=0, tiled=True)


def local(strips, index, shift, flags):
    strips = jnp.transpose(strips, (1, 0, 2))
    index = index.reshape(1, -1)
    (first,) = bucket(first_kernel, (), strips, index)
    table = (8, flags.shape[0])
    extra = (jax.ShapeDtypeStruct(table, jnp.int32), jax.ShapeDtypeStruct(table, F32))
    second, near, wide = bucket(second_kernel, extra, strips, index, flags.reshape(1, -1))
    recv = exchange(first)
    q = exchange(second)
    parts = chol(recv, shift, wide)
    return last(near, recv, q, shift, *parts)


def solution(mesh):
    in_specs = (P(AXES, None, None), P(AXES, None), P(AXES, None), P())
    out_specs = (P(AXES, None, None, None), P(AXES, None, None, None))
    return jax.shard_map(local, mesh=mesh, in_specs=in_specs, out_specs=out_specs, check_vma=False)
```
